32 devices in a mesh: gx: 8 (over y, x, core), gy: 4 (over z).
Axes of the slice: x: 2, y: 2, z: 4, core: 2. Of those that a mesh axis runs over, the one named last changes fastest.
Arguments:
- rhs: float32 [8, 125, 512], P('gx', None, 'gy'), may hold values from -6 to 6
- inverse: bfloat16 [8, 125, 125, 512], P('gx', None, None, 'gy')
- weights: float32 [8, 4, 512], P('gx', None, 'gy'), may hold values from 0.12 to 0.3
- neighbours: int32 [8, 4, 512], P('gx', None, 'gy'), may hold values from 0 to 383, as said below
- send_lists: int32 [8, 4, 256], P('gx', None, 'gy'), may hold values from 0 to 127
- coloring: int32 [8, 4], P('gx', 'gy'), may hold values from 0 to 3, as said below
Outputs:
- solution: float32 [8, 125, 512], P('gx', None, 'gy')
- norms: float32 [2], replicated
The draws below stay inside these ranges and needn't reach their ends.
Inputs may be any that keep to these rules, and one draw needn't show every extreme that they name: `coloring`: the color of subdomain (i, j) depends only on i mod 2 and j mod 2, and the four parity classes have four different colors; which class has which color varies. `neighbours`: slots below 128 are the subdomain's own faces, the rest the received intersection faces in the order of the steps; every received slot is used by some face.
All inputs are finite; a program needn't handle non-finite values.
Results may differ from the reference program's by a relative error of at most 0.0055.
Values sent between devices are 32-bit elements; how exact they have to be, the bound alone decides.
No kernel may reach another device: no remote copies, remote signals or barrier semaphores. Data moves between devices by JAX's collectives and lax.ppermute only.
A program may use at most 64 MiB of HBM per device.

```python
import math
import jax
import jax.numpy as jnp
from jax import lax

ROWS = 125
FACES = 128
HALO = 64
NEIGH = 4
SWEEPS = 2
N_GX = 8
N_GY = 4


def draw_inverse(key, part):
    first, second = jax.random.split(key)
    shape = (N_GX, ROWS, ROWS, N_GY * FACES)
    spread = 0.02 * jax.random.normal(first, shape, jnp.float32)
    diagonal = jax.random.uniform(second, (N_GX, 1, 1, N_GY * FACES), jnp.float32, 0.5, 0.9)
    unit = jnp.eye(ROWS, dtype=jnp.float32)[None, :, :, None]
    return (spread * (1.0 - unit) + unit * diagonal).astype(jnp.bfloat16)


def one_device(key):
    first, second = jax.random.split(key)
    order = jax.random.permutation(first, 2 * FACES).astype(jnp.int32)
    lead = jnp.stack([FACES + order[:FACES], FACES + order[FACES:]])
    rest = jax.random.randint(second, (NEIGH - 2, FACES), 0, 3 * FACES).astype(jnp.int32)
    return jnp.concatenate([lead, rest], axis=0)


def draw_neighbours(key, part):
    keys = jax.random.split(jax.random.fold_in(key, 7), N_GX * N_GY)
    tables = jax.vmap(one_device)(keys)
    tables = tables.reshape(N_GX, N_GY, NEIGH, FACES).transpose(0, 2, 1, 3)
    return tables.reshape(N_GX, NEIGH, N_GY * FACES).astype(jnp.int32)


def draw_coloring(key, part):
    order = jax.random.permutation(jax.random.fold_in(key, 11), 4).astype(jnp.int32)
    first = (jnp.arange(N_GX, dtype=jnp.int32) % 2)[:, None]
    second = (jnp.arange(N_GY, dtype=jnp.int32) % 2)[None, :]
    return order[first * 2 + second].astype(jnp.int32)


def plant(drawn, key, low, largest):
    spot = [jax.random.randint(jax.random.fold_in(key, axis), (), 0, length) for axis, length in enumerate(drawn.shape)]
    widest = drawn.shape.index(max(drawn.shape))
    neighbour = spot[:widest] + [(spot[widest] + 1) % drawn.shape[widest]] + spot[widest + 1:]
    return drawn.at[tuple(spot)].set(low).at[tuple(neighbour)].set(largest)


def level_of(key, shape, cuts, low, largest):
    factor_of, own = 1.0, jax.random.fold_in(key, 6)
    for dim, blocks in cuts:
        draws = jnp.exp(jax.random.uniform(jax.random.fold_in(own, dim), (blocks,), jnp.float32, low / len(cuts), largest / len(cuts)))
        factor_of = factor_of * jnp.repeat(draws, shape[dim] // blocks).reshape([-1 if axis == dim else 1 for axis in range(len(shape))])
    return factor_of


def normal_values(own_key, dims, scale, limit, shards=(), kind=jnp.bfloat16):
    result = scale * jax.random.normal(own_key, dims, jnp.float32)
    if shards:
        result = result * level_of(own_key, dims, shards, -0.22, 0.18)
    return jnp.clip(result, -limit, limit).astype(kind)


def setup_inputs(seed: int = 0) -> dict:
    seeds = jax.random.split(jax.random.key(seed), 7)
    return {
        "rhs": normal_values(seeds[0], (N_GX, ROWS, N_GY * FACES), 1.0, 6.0, ((0, 8), (2, 4)), jnp.float32),
        "inverse": draw_inverse(jax.random.fold_in(seeds[6], 71), 0),
        "weights": jnp.clip(jnp.exp(math.log(0.3) - 0.9162908 * jax.random.uniform(seeds[2], (N_GX, NEIGH, N_GY * FACES), jnp.float32) ** level_of(seeds[2], (N_GX, NEIGH, N_GY * FACES), ((0, 8), (2, 4)), -0.2, 0.2)), 0.12, 0.3),
        "neighbours": draw_neighbours(jax.random.fold_in(seeds[6], 71), 0),
        "send_lists": plant(jax.random.randint(seeds[4], (N_GX, 4, N_GY * HALO), 0, FACES), jax.random.fold_in(seeds[4], 1), 0, FACES - 1).astype(jnp.int32),
        "coloring": draw_coloring(jax.random.fold_in(seeds[6], 71), 0),
    }


def apply_rows(pair):
    block, source = pair
    return jnp.einsum('ijyf,jyf->iyf', block.astype(jnp.float32), source.astype(jnp.float32))

def reference(rhs, inverse, weights, neighbours, send_lists, coloring):
    halo_faces = FACES // 2
    right = rhs.reshape(N_GX, ROWS, N_GY, FACES)
    coupling = weights.reshape(N_GX, NEIGH, N_GY, FACES)
    slots = neighbours.reshape(N_GX, NEIGH, N_GY, FACES)
    sending = send_lists.reshape(N_GX, 4, N_GY, halo_faces)
    blocks = inverse.reshape(N_GX, ROWS, ROWS, N_GY, FACES)
    solution = jnp.zeros((N_GX, ROWS, N_GY, FACES), jnp.float32)
    zero_rows = jnp.zeros((1, ROWS, N_GY, halo_faces), jnp.float32)
    zero_cols = jnp.zeros((N_GX, ROWS, 1, halo_faces), jnp.float32)
    results = []
    for sweep in range(SWEEPS):
        squares = jnp.zeros((), jnp.float32)
        for color in range(4):
            packs = []
            for side in range(4):
                index = jnp.broadcast_to(sending[:, side][:, None], (N_GX, ROWS, N_GY, halo_faces))
                packs.append(jnp.take_along_axis(solution, index, axis=3))
            below = jnp.concatenate([zero_rows, packs[0][:-1]], axis=0)
            above = jnp.concatenate([packs[1][1:], zero_rows], axis=0)
            left = jnp.concatenate([zero_cols, packs[2][:, :, :-1]], axis=2)
            right_side = jnp.concatenate([packs[3][:, :, 1:], zero_cols], axis=2)
            extended = jnp.concatenate([solution, below, above, left, right_side], axis=3)
            couple = jnp.zeros_like(solution)
            for k in range(NEIGH):
                index = jnp.broadcast_to(slots[:, k][:, None], (N_GX, ROWS, N_GY, FACES))
                couple = couple + coupling[:, k][:, None] * jnp.take_along_axis(extended, index, axis=3)
            source = (right + couple).astype(jnp.bfloat16)
            candidate = lax.map(apply_rows, (blocks, source))
            active = (coloring == color)[:, None, :, None]
            delta = jnp.where(active, candidate - solution, 0.0)
            squares = squares + jnp.sum(delta * delta)
            solution = jnp.where(active, candidate, solution)
        results.append(jnp.sqrt(squares))
    return (solution.reshape(N_GX, ROWS, N_GY * FACES), jnp.stack(results))
```

```python
import jax
import jax.numpy as jnp
from jax import lax
from jax.experimental import pallas as pl
from jax.experimental.pallas import tpu as pltpu
from jax.sharding import PartitionSpec as P

LANES = 128
SUB = 8
GROUP = 25
VMEM_LIMIT = 16 * 1024 * 1024
CHUNKS = 5
HELD = 3
FIRST, SECOND, CONTROL = range(3)

VSPEC = pl.BlockSpec(memory_space=pltpu.VMEM)
SSPEC = pl.BlockSpec(memory_space=pltpu.SMEM)


def vmem(value):
    return pltpu.with_memory_space_constraint(value, pltpu.VMEM)


def hbm(value):
    return pltpu.with_memory_space_constraint(value, pltpu.HBM)


def smem(value):
    return pltpu.with_memory_space_constraint(value, pltpu.SMEM)


class Plan:
    def __init__(self, mesh, rows, faces, halo, neigh):
        self.nx, self.ny = mesh.shape["gx"], mesh.shape["gy"]
        self.rows, self.faces, self.halo, self.neigh = rows, faces, halo, neigh
        assert self.nx % 2 == 0 and self.ny % 2 == 0
        assert faces == LANES and 2 * halo == LANES
        self.tiles = -(-rows // (2 * SUB)) * 2
        self.pad = self.tiles * SUB
        self.half = self.pad // 2
        assert rows % CHUNKS == 0
        self.chunk = rows // CHUNKS
        self.along = (self.pad, 2 * self.pad)
        self.rhs = 3 * self.pad
        self.norm = 4 * self.pad
        self.step = self.norm + 2 * SUB
        self.state = self.step + SUB
        self.state_type = pltpu.VMEM((self.state, LANES), jnp.float32)
        self.pack_type = pltpu.VMEM((self.half, LANES), jnp.float32)
        self.control_type = pltpu.SMEM((CONTROL,), jnp.int32)

    def held_type(self, inverse):
        return pltpu.VMEM((HELD * self.chunk, *inverse.shape[1:]), inverse.dtype)

    def rest_type(self, inverse):
        return pltpu.VMEM(((CHUNKS - HELD) * self.chunk, *inverse.shape[1:]), inverse.dtype)


def write_pack(plan, state, lists, row, ref):
    low = lax.broadcasted_iota(jnp.int32, (SUB, LANES), 1) < plan.halo
    index = jnp.broadcast_to(lists[pl.ds(row, 1), :], (SUB, LANES))

    def take(t):
        tile = state[t * SUB:(t + 1) * SUB, :]
        return jnp.take_along_axis(tile, index, axis=1, mode="promise_in_bounds")

    for t in range(plan.tiles // 2):
        ref[t * SUB:(t + 1) * SUB, :] = jnp.where(low, take(t), take(t + plan.tiles // 2))


def merge(plan, state, base, even, odd):
    low = lax.broadcasted_iota(jnp.int32, (SUB, LANES), 1) < plan.halo
    for t in range(plan.tiles // 2):
        a = even[t * SUB:(t + 1) * SUB, :]
        b = odd[t * SUB:(t + 1) * SUB, :]
        first = jnp.where(low, a, pltpu.roll(b, plan.halo, 1))
        second = jnp.where(low, pltpu.roll(a, plan.halo, 1), b)
        state[pl.ds(base + t * SUB, SUB), :] = first
        state[pl.ds(base + plan.half + t * SUB, SUB), :] = second


def apply_inverse(plan, blocks, source, result, base, start, stop):
    src = source[0:plan.rows, :]
    group = max(g for g in range(1, GROUP + 1) if (stop - start) % g == 0)

    def step(n, carry):
        for k in range(group):
            i = start + n * group + k
            block = blocks[i].astype(jnp.float32)
            result[pl.ds(base + i, 1), :] = jnp.sum(block * src, axis=0, keepdims=True)
        return carry

    lax.fori_loop(0, (stop - start) // group, step, 0)


def chunk_copies(plan, inverse, kept, rest, sems, first):
    copies = []
    for n in range(first, CHUNKS):
        part = inverse.at[pl.ds(n * plan.chunk, plan.chunk)]
        ref, at = (kept, n) if n < HELD else (rest, n - HELD)
        copies.append(pltpu.make_async_copy(part, ref.at[pl.ds(at * plan.chunk, plan.chunk)], sems.at[n]))
    return copies


def apply_chunks(plan, kept, rest, source, result, start, stop):
    held = HELD * plan.chunk
    if start < HELD:
        apply_inverse(plan, kept, source, result, 0, start * plan.chunk, min(stop, HELD) * plan.chunk)
    if stop > HELD:
        apply_inverse(plan, rest, source, result, held, max(start - HELD, 0) * plan.chunk, (stop - HELD) * plan.chunk)


def parts_of(value):
    high = value.astype(jnp.bfloat16)
    low = (value - high.astype(jnp.float32)).astype(jnp.bfloat16)
    return high, low


def update(plan, second, state, coupling, inverse, kept, rest, source, result, sems):
    copies = chunk_copies(plan, inverse, kept, rest, sems, HELD)
    for c in copies:
        c.start()
    pad = plan.pad
    values = jnp.concatenate([state[n * pad:(n + 1) * pad, :] for n in range(3)], axis=1)
    high, low = parts_of(values)
    size = 3 * LANES
    couple = jnp.dot(high, coupling[0:size, :], preferred_element_type=jnp.float32)
    couple = couple + jnp.dot(low, coupling[0:size, :], preferred_element_type=jnp.float32)
    couple = couple + jnp.dot(high, coupling[size:2 * size, :], preferred_element_type=jnp.float32)
    right = state[plan.rhs:plan.rhs + pad, :]
    source[...] = (right + couple).astype(jnp.bfloat16).astype(jnp.float32)
    result[pad - SUB:pad, :] = jnp.zeros((SUB, LANES), jnp.float32)
    apply_chunks(plan, kept, rest, source, result, 0, HELD)
    for c in copies:
        c.wait()
    apply_chunks(plan, kept, rest, source, result, HELD, CHUNKS)
    finish(plan, second, state, result)


def finish(plan, second, state, result):
    squares = jnp.zeros((SUB, LANES), jnp.float32)
    for t in range(plan.tiles):
        new = result[t * SUB:(t + 1) * SUB, :]
        delta = new - state[t * SUB:(t + 1) * SUB, :]
        squares = squares + delta * delta
        state[t * SUB:(t + 1) * SUB, :] = new
    state[pl.ds(pl.multiple_of(plan.norm + second * SUB, SUB), SUB), :] = squares


def first_kernel(plan):
    rows, pad, neigh = plan.rows, plan.pad, plan.neigh

    def kernel(color, color_x, color_y, rhs, weights, neighbours, lists, inverse,
               code, control, kept, state, coupling, table, xe, xo, ye, yo,
               cx, cy, rhs_v, weights_v, slots_v, lists_v, rest, source, result, sems, part_sems):
        moves = ((color_x, cx), (color_y, cy), (neighbours, slots_v), (weights, weights_v),
                 (lists, lists_v), (rhs, rhs_v))
        copies = [pltpu.make_async_copy(a, b, sems.at[n]) for n, (a, b) in enumerate(moves)]
        parts = chunk_copies(plan, inverse, kept, rest, part_sems, 0)
        for c in copies + parts:
            c.start()
        odd_x = lax.axis_index("gx") & 1
        odd_y = lax.axis_index("gy") & 1
        state[...] = jnp.zeros(state.shape, jnp.float32)
        for c in copies[:2]:
            c.wait()
        mine, beside_x, beside_y = color[0, 0], cx[0, 0], cy[0, 0]
        across = 6 - mine - beside_x - beside_y
        to_x = jnp.logical_or(beside_x == 0, across == 0).astype(jnp.int32)
        to_y = jnp.logical_or(beside_y == 0, across == 0).astype(jnp.int32)
        zero_x, zero_y = odd_x ^ to_x, odd_y ^ to_y
        opposite = jnp.where(to_x == 0, jnp.where(to_y == 0, across, beside_x), jnp.where(to_y == 0, beside_y, mine))
        next_x = jnp.where(to_x == 0, jnp.where(to_y == 0, beside_x, across), jnp.where(to_y == 0, mine, beside_y))
        chain = opposite == 2
        first = jnp.where(chain, mine, jnp.where(opposite == 1, mine >> 1, (mine + 1) >> 1))
        control[FIRST] = first
        control[SECOND] = first + jnp.where(chain, 4, 2)
        red = zero_x ^ zero_y
        total = 0
        for n in range(7):
            step = n >> 1 & 1
            alternate = jnp.where(n < jnp.where(opposite == 1, 3, 4), 5 + (red ^ (n & 1)), 0)
            axis_x = 1 + 2 * (zero_x ^ step)
            axis_y = 2 + 2 * (zero_y ^ step)
            around = jnp.where((next_x == 1) == (n % 2 == 0), axis_x, axis_y)
            total = total + (jnp.where(chain, around, alternate) << (4 * n))
        code[0] = total

        for c in copies[2:]:
            c.wait()
        state[plan.rhs:plan.rhs + rows, :] = rhs_v[:, 0, :]
        source[...] = state[plan.rhs:plan.rhs + pad, :].astype(jnp.bfloat16).astype(jnp.float32)

        slots = slots_v[...]
        group = (slots - plan.faces) // plan.halo
        within = (slots - plan.faces) & (plan.halo - 1)
        along_y = (group >= 2).astype(jnp.int32)
        side = ((group & 1) + 1 + jnp.where(group >= 2, odd_y, odd_x)) & 1
        place = jnp.where(slots < plan.faces, slots, plan.faces * (1 + along_y) + within + plan.halo * side)
        size = 3 * LANES
        where = lax.broadcasted_iota(jnp.int32, (size, LANES), 0)
        total = jnp.zeros((size, LANES), jnp.float32)
        for k in range(neigh):
            total = total + jnp.where(where == place[k:k + 1, :], weights_v[k:k + 1, :], 0.0)
        coupling[0:size, :], coupling[size:2 * size, :] = parts_of(total)

        both = jnp.concatenate([lists_v[...], lists_v[...]], axis=1)
        table[...] = jnp.zeros(table.shape, jnp.int32)
        for n, odd in ((0, odd_x), (2, odd_y)):
            table[n:n + 1, :] = jnp.where(odd == 0, both[n:n + 1], both[n + 1:n + 2])
            table[n + 1:n + 2, :] = jnp.where(odd == 0, both[n + 1:n + 2], both[n:n + 1])

        result[pad - SUB:pad, :] = jnp.zeros((SUB, LANES), jnp.float32)
        for n in range(CHUNKS):
            parts[n].wait()

            @pl.when(first == 0)
            def _():
                apply_chunks(plan, kept, rest, source, result, n, n + 1)

        @pl.when(first == 0)
        def _():
            finish(plan, 0, state, result)

        for n, ref in enumerate((xe, xo, ye, yo)):
            write_pack(plan, state, table, n, ref)

    def call(color, color_x, color_y, rhs, weights, neighbours, lists, inverse):
        return pl.pallas_call(
            kernel,
            name="first",
            in_specs=[SSPEC, pl.BlockSpec(memory_space=pl.ANY), pl.BlockSpec(memory_space=pl.ANY)]
            + [pl.BlockSpec(memory_space=pltpu.HBM)] * 5,
            out_specs=[SSPEC] * 2 + [VSPEC] * 8,
            out_shape=[
                pltpu.SMEM((1,), jnp.int32),
                plan.control_type,
                plan.held_type(inverse),
                plan.state_type,
                pltpu.VMEM((6 * LANES, LANES), jnp.bfloat16),
                pltpu.VMEM((SUB, LANES), jnp.int32),
            ] + [plan.pack_type] * 4,
            compiler_params=pltpu.CompilerParams(vmem_limit_bytes=VMEM_LIMIT),
            scratch_shapes=[
                pltpu.SMEM(color.shape, color.dtype),
                pltpu.SMEM(color.shape, color.dtype),
                pltpu.VMEM(rhs.shape, rhs.dtype),
                pltpu.VMEM(weights.shape, weights.dtype),
                pltpu.VMEM(neighbours.shape, neighbours.dtype),
                pltpu.VMEM(lists.shape, lists.dtype),
                plan.rest_type(inverse),
                pltpu.VMEM((pad, LANES), jnp.float32),
                pltpu.VMEM((pad, LANES), jnp.float32),
                pltpu.SemaphoreType.DMA((6,)),
                pltpu.SemaphoreType.DMA((CHUNKS,)),
            ],
        )(color, color_x, color_y, *(hbm(v) for v in (rhs, weights, neighbours, lists, inverse)))

    return call


def merge_kernel(plan, name, receives, axes):
    def kernel(*refs):
        old_state, *got = refs[:-1]
        state = refs[-1]
        del old_state
        odd_x = lax.axis_index("gx") & 1
        odd_y = lax.axis_index("gy") & 1

        @pl.when(receives(odd_x, odd_y))
        def _():
            for n, axis in enumerate(axes):
                merge(plan, state, plan.along[axis], got[2 * n], got[2 * n + 1])

    def call(state, got):
        return pl.pallas_call(
            kernel,
            name=name,
            in_specs=[VSPEC] * (1 + len(got)),
            out_specs=VSPEC,
            out_shape=plan.state_type,
            input_output_aliases={0: 0},
            compiler_params=pltpu.CompilerParams(vmem_limit_bytes=VMEM_LIMIT),
        )(*(vmem(v) for v in (state, *got)))

    return call


def level_kernel(plan):
    def kernel(control, old_state, coupling, table, kept, inverse, state, xe, xo, ye, yo, rest, source, result, sems):
        del old_state
        steps = state[plan.step:plan.step + SUB, :] + 1.0
        state[plan.step:plan.step + SUB, :] = steps
        step = steps[0, 0].astype(jnp.int32)
        second = (step == control[SECOND]).astype(jnp.int32)
        turn = jnp.logical_or(step == control[FIRST], step == control[SECOND])

        @pl.when(turn)
        def _():
            update(plan, second, state, coupling, inverse, kept, rest, source, result, sems)

        for n, ref in enumerate((xe, xo, ye, yo)):
            write_pack(plan, state, table, n, ref)

    def call(control, state, coupling, table, kept, inverse):
        return pl.pallas_call(
            kernel,
            name="level",
            in_specs=[SSPEC] + [VSPEC] * 4 + [pl.BlockSpec(memory_space=pltpu.HBM)],
            out_specs=[VSPEC] * 5,
            out_shape=[plan.state_type] + [plan.pack_type] * 4,
            input_output_aliases={1: 0},
            compiler_params=pltpu.CompilerParams(vmem_limit_bytes=VMEM_LIMIT),
            scratch_shapes=[
                plan.rest_type(inverse),
                pltpu.VMEM((plan.pad, LANES), jnp.float32),
                pltpu.VMEM((plan.pad, LANES), jnp.float32),
                pltpu.SemaphoreType.DMA((CHUNKS,)),
            ],
        )(smem(control), *(vmem(v) for v in (state, coupling, table, kept)), hbm(inverse))

    return call


def last_kernel(plan):
    devices = plan.nx * plan.ny

    def kernel(state, out, sums):
        out[:, 0, :] = state[0:plan.rows, :]
        lane = lax.broadcasted_iota(jnp.int32, (devices, LANES), 1)
        first = jnp.sum(state[plan.norm:plan.norm + SUB, :])
        second = jnp.sum(state[plan.norm + SUB:plan.norm + 2 * SUB, :])
        sums[...] = jnp.where(lane == 0, first, jnp.where(lane == 1, second, 0.0))

    def call(state):
        return pl.pallas_call(
            kernel,
            name="last",
            in_specs=[VSPEC],
            out_specs=[VSPEC] * 2,
            out_shape=[
                pltpu.VMEM((plan.rows, 1, LANES), jnp.float32),
                pltpu.VMEM((devices, LANES), jnp.float32),
            ],
            compiler_params=pltpu.CompilerParams(vmem_limit_bytes=VMEM_LIMIT),
        )(vmem(state))

    return call


def edge_pairs(plan, axis, odd, sends, both):
    pairs = []
    for i in range(plan.nx):
        for j in range(plan.ny):
            u, v = (i + 1, j) if axis == 0 else (i, j + 1)
            if (i, j)[axis] % 2 != odd or u >= plan.nx or v >= plan.ny:
                continue
            here, there = i * plan.ny + j, u * plan.ny + v
            if both or sends(i, j):
                pairs.append((here, there))
            if both or sends(u, v):
                pairs.append((there, here))
    return pairs


def flow(plan, name, axes, parity):
    steps = [(axis, odd) for axis in axes for odd in (0, 1)]

    def sends(i, j):
        return (i * (0 in axes) + j * (1 in axes)) % 2 == parity

    def receives(i, j):
        return ((i if axes == (0,) else j if axes == (1,) else i ^ j) & 1) != parity

    def run(state, *packs):
        got = []
        for n, (axis, odd) in enumerate(steps):
            pairs = edge_pairs(plan, axis, odd, sends, n == len(steps) - 1)
            got.append(lax.ppermute(packs[2 * axis + odd], ("gx", "gy"), pairs))
        return merge_kernel(plan, name, receives, axes)(state, got)

    return run


def body_for(mesh):
    def body(rhs, inverse, weights, neighbours, send_lists, coloring):
        rows, faces = rhs.shape[1:]
        plan = Plan(mesh, rows, faces, send_lists.shape[2], weights.shape[1])
        color_x = lax.ppermute(coloring, "gx", [(i, i ^ 1) for i in range(plan.nx)])
        color_y = lax.ppermute(coloring, "gy", [(j, j ^ 1) for j in range(plan.ny)])
        code, control, kept, state, coupling, table, *packs = first_kernel(plan)(
            coloring, color_x, color_y, rhs.transpose(1, 0, 2), weights[0], neighbours[0], send_lists[0], inverse[0])
        flows = [
            flow(plan, "along_x0", (0,), 0),
            flow(plan, "along_y0", (1,), 0),
            flow(plan, "along_x1", (0,), 1),
            flow(plan, "along_y1", (1,), 1),
            flow(plan, "both0", (0, 1), 0),
            flow(plan, "both1", (0, 1), 1),
        ]

        def turn(carry):
            code, state, packs = carry
            state = lax.switch((code & 7) - 1, flows, state, *packs)
            state, *packs = level_kernel(plan)(control, state, coupling, table, kept, inverse[0])
            return code >> 4, state, tuple(packs)

        state = lax.while_loop(lambda carry: carry[0] != 0, turn, (code[0], state, tuple(packs)))[1]
        out, sums = last_kernel(plan)(state)
        sums = lax.all_to_all(sums, ("gx", "gy"), 0, 0, tiled=True)
        norms = jnp.sqrt(jnp.sum(sums[:, :2], axis=0))
        return out.transpose(1, 0, 2), norms

    return body


def solution(mesh):
    in_specs = (
        P("gx", None, "gy"),
        P("gx", None, None, "gy"),
        P("gx", None, "gy"),
        P("gx", None, "gy"),
        P("gx", None, "gy"),
        P("gx", "gy"),
    )
    out_specs = (P("gx", None, "gy"), P())
    return jax.shard_map(body_for(mesh), mesh=mesh, in_specs=in_specs, out_specs=out_specs, check_vma=False)
```

```python
import jax
import jax.numpy as jnp
from jax import lax
from jax.experimental import pallas as pl
from jax.experimental.pallas import tpu as pltpu
from jax.sharding import PartitionSpec as P

LANES = 128
SUB = 8
GROUP = 25
VMEM_LIMIT = 16 * 1024 * 1024
CHUNKS = 5
HELD = 3
FIRST, SECOND, CONTROL = range(3)

VSPEC = pl.BlockSpec(memory_space=pltpu.VMEM)
SSPEC = pl.BlockSpec(memory_space=pltpu.SMEM)


def vmem(value):
    return pltpu.with_memory_space_constraint(value, pltpu.VMEM)


def hbm(value):
    return pltpu.with_memory_space_constraint(value, pltpu.HBM)


def smem(value):
    return pltpu.with_memory_space_constraint(value, pltpu.SMEM)


class Plan:
    def __init__(self, mesh, rows, faces, halo, neigh):
        self.nx, self.ny = mesh.shape["gx"], mesh.shape["gy"]
        self.rows, self.faces, self.halo, self.neigh = rows, faces, halo, neigh
        assert self.nx % 2 == 0 and self.ny % 2 == 0
        assert faces == LANES and 2 * halo == LANES
        self.tiles = -(-rows // (2 * SUB)) * 2
        self.pad = self.tiles * SUB
        self.half = self.pad // 2
        assert rows % CHUNKS == 0
        self.chunk = rows // CHUNKS
        self.along = (self.pad, 2 * self.pad)
        self.rhs = 3 * self.pad
        self.norm = 4 * self.pad
        self.step = self.norm + 2 * SUB
        self.state = self.step + SUB
        self.state_type = pltpu.VMEM((self.state, LANES), jnp.float32)
        self.pack_type = pltpu.VMEM((self.half, LANES), jnp.float32)
        self.control_type = pltpu.SMEM((CONTROL,), jnp.int32)

    def held_type(self, inverse):
        return pltpu.VMEM((HELD * self.chunk, *inverse.shape[1:]), inverse.dtype)

    def rest_type(self, inverse):
        return pltpu.VMEM(((CHUNKS - HELD) * self.chunk, *inverse.shape[1:]), inverse.dtype)


def write_pack(plan, state, lists, row, ref):
    low = lax.broadcasted_iota(jnp.int32, (SUB, LANES), 1) < plan.halo
    index = jnp.broadcast_to(lists[pl.ds(row, 1), :], (SUB, LANES))

    def take(t):
        tile = state[t * SUB:(t + 1) * SUB, :]
        return jnp.take_along_axis(tile, index, axis=1, mode="promise_in_bounds")

    for t in range(plan.tiles // 2):
        ref[t * SUB:(t + 1) * SUB, :] = jnp.where(low, take(t), take(t + plan.tiles // 2))


def merge(plan, state, base, even, odd):
    low = lax.broadcasted_iota(jnp.int32, (SUB, LANES), 1) < plan.halo
    for t in range(plan.tiles // 2):
        a = even[t * SUB:(t + 1) * SUB, :]
        b = odd[t * SUB:(t + 1) * SUB, :]
        first = jnp.where(low, a, pltpu.roll(b, plan.halo, 1))
        second = jnp.where(low, pltpu.roll(a, plan.halo, 1), b)
        state[pl.ds(base + t * SUB, SUB), :] = first
        state[pl.ds(base + plan.half + t * SUB, SUB), :] = second


def apply_inverse(plan, blocks, source, result, base, start, stop):
    src = source[0:plan.rows, :]
    group = max(g for g in range(1, GROUP + 1) if (stop - start) % g == 0)

    def step(n, carry):
        for k in range(group):
            i = start + n * group + k
            block = blocks[i].astype(jnp.float32)
            result[pl.ds(base + i, 1), :] = jnp.sum(block * src, axis=0, keepdims=True)
        return carry

    lax.fori_loop(0, (stop - start) // group, step, 0)


def chunk_copies(plan, inverse, kept, rest, sems, first):
    copies = []
    for n in range(first, CHUNKS):
        part = inverse.at[pl.ds(n * plan.chunk, plan.chunk)]
        ref, at = (kept, n) if n < HELD else (rest, n - HELD)
        copies.append(pltpu.make_async_copy(part, ref.at[pl.ds(at * plan.chunk, plan.chunk)], sems.at[n]))
    return copies


def apply_chunks(plan, kept, rest, source, result, start, stop):
    held = HELD * plan.chunk
    if start < HELD:
        apply_inverse(plan, kept, source, result, 0, start * plan.chunk, min(stop, HELD) * plan.chunk)
    if stop > HELD:
        apply_inverse(plan, rest, source, result, held, max(start - HELD, 0) * plan.chunk, (stop - HELD) * plan.chunk)


def parts_of(value):
    high = value.astype(jnp.bfloat16)
    low = (value - high.astype(jnp.float32)).astype(jnp.bfloat16)
    return high, low


def update(plan, second, state, coupling, inverse, kept, rest, source, result, sems):
    copies = chunk_copies(plan, inverse, kept, rest, sems, HELD)
    for c in copies:
        c.start()
    pad = plan.pad
    values = jnp.concatenate([state[n * pad:(n + 1) * pad, :] for n in range(3)], axis=1)
    high, low = parts_of(values)
    size = 3 * LANES
    couple = jnp.dot(high, coupling[0:size, :], preferred_element_type=jnp.float32)
    couple = couple + jnp.dot(low, coupling[0:size, :], preferred_element_type=jnp.float32)
    couple = couple + jnp.dot(high, coupling[size:2 * size, :], preferred_element_type=jnp.float32)
    right = state[plan.rhs:plan.rhs + pad, :]
    source[...] = (right + couple).astype(jnp.bfloat16).astype(jnp.float32)
    result[pad - SUB:pad, :] = jnp.zeros((SUB, LANES), jnp.float32)
    apply_chunks(plan, kept, rest, source, result, 0, HELD)
    for c in copies:
        c.wait()
    apply_chunks(plan, kept, rest, source, result, HELD, CHUNKS)
    finish(plan, second, state, result)


def finish(plan, second, state, result):
    squares = jnp.zeros((SUB, LANES), jnp.float32)
    for t in range(plan.tiles):
        new = result[t * SUB:(t + 1) * SUB, :]
        delta = new - state[t * SUB:(t + 1) * SUB, :]
        squares = squares + delta * delta
        state[t * SUB:(t + 1) * SUB, :] = new
    state[pl.ds(pl.multiple_of(plan.norm + second * SUB, SUB), SUB), :] = squares


def first_kernel(plan):
    rows, pad, neigh = plan.rows, plan.pad, plan.neigh

    def kernel(color, color_x, color_y, rhs, weights, neighbours, lists, inverse,
               code, control, kept, state, coupling, table, xe, xo, ye, yo,
               cx, cy, rhs_v, weights_v, slots_v, lists_v, rest, source, result, sems, part_sems):
        moves = ((color_x, cx), (color_y, cy), (neighbours, slots_v), (weights, weights_v),
                 (lists, lists_v), (rhs, rhs_v))
        copies = [pltpu.make_async_copy(a, b, sems.at[n]) for n, (a, b) in enumerate(moves)]
        parts = chunk_copies(plan, inverse, kept, rest, part_sems, 0)
        for c in copies + parts:
            c.start()
        odd_x = lax.axis_index("gx") & 1
        odd_y = lax.axis_index("gy") & 1
        state[...] = jnp.zeros(state.shape, jnp.float32)
        for c in copies[:2]:
            c.wait()
        mine, beside_x, beside_y = color[0, 0], cx[0, 0], cy[0, 0]
        across = 6 - mine - beside_x - beside_y
        to_x = jnp.logical_or(beside_x == 0, across == 0).astype(jnp.int32)
        to_y = jnp.logical_or(beside_y == 0, across == 0).astype(jnp.int32)
        zero_x, zero_y = odd_x ^ to_x, odd_y ^ to_y
        opposite = jnp.where(to_x == 0, jnp.where(to_y == 0, across, beside_x), jnp.where(to_y == 0, beside_y, mine))
        next_x = jnp.where(to_x == 0, jnp.where(to_y == 0, beside_x, across), jnp.where(to_y == 0, mine, beside_y))
        chain = opposite == 2
        first = jnp.where(chain, mine, jnp.where(opposite == 1, mine >> 1, (mine + 1) >> 1))
        control[FIRST] = first
        control[SECOND] = first + jnp.where(chain, 4, 2)
        red = zero_x ^ zero_y
        total = 0
        for n in range(7):
            step = n >> 1 & 1
            alternate = jnp.where(n < jnp.where(opposite == 1, 3, 4), 5 + (red ^ (n & 1)), 0)
            axis_x = 1 + 2 * (zero_x ^ step)
            axis_y = 2 + 2 * (zero_y ^ step)
            around = jnp.where((next_x == 1) == (n % 2 == 0), axis_x, axis_y)
            total = total + (jnp.where(chain, around, alternate) << (4 * n))
        code[0] = total

        for c in copies[2:]:
            c.wait()
        state[plan.rhs:plan.rhs + rows, :] = rhs_v[:, 0, :]
        source[...] = state[plan.rhs:plan.rhs + pad, :].astype(jnp.bfloat16).astype(jnp.float32)

        slots = slots_v[...]
        group = (slots - plan.faces) // plan.halo
        within = (slots - plan.faces) & (plan.halo - 1)
        along_y = (group >= 2).astype(jnp.int32)
        side = ((group & 1) + 1 + jnp.where(group >= 2, odd_y, odd_x)) & 1
        place = jnp.where(slots < plan.faces, slots, plan.faces * (1 + along_y) + within + plan.halo * side)
        size = 3 * LANES
        where = lax.broadcasted_iota(jnp.int32, (size, LANES), 0)
        total = jnp.zeros((size, LANES), jnp.float32)
        for k in range(neigh):
            total = total + jnp.where(where == place[k:k + 1, :], weights_v[k:k + 1, :], 0.0)
        coupling[0:size, :], coupling[size:2 * size, :] = parts_of(total)

        both = jnp.concatenate([lists_v[...], lists_v[...]], axis=1)
        table[...] = jnp.zeros(table.shape, jnp.int32)
        for n, odd in ((0, odd_x), (2, odd_y)):
            table[n:n + 1, :] = jnp.where(odd == 0, both[n:n + 1], both[n + 1:n + 2])
            table[n + 1:n + 2, :] = jnp.where(odd == 0, both[n + 1:n + 2], both[n:n + 1])

        result[pad - SUB:pad, :] = jnp.zeros((SUB, LANES), jnp.float32)
        for n in range(CHUNKS):
            parts[n].wait()

            @pl.when(first == 0)
            def _():
                apply_chunks(plan, kept, rest, source, result, n, n + 1)

        @pl.when(first == 0)
        def _():
            finish(plan, 0, state, result)

        for n, ref in enumerate((xe, xo, ye, yo)):
            write_pack(plan, state, table, n, ref)

    def call(color, color_x, color_y, rhs, weights, neighbours, lists, inverse):
        return pl.pallas_call(
            kernel,
            name="first",
            in_specs=[SSPEC, pl.BlockSpec(memory_space=pl.ANY), pl.BlockSpec(memory_space=pl.ANY)]
            + [pl.BlockSpec(memory_space=pltpu.HBM)] * 5,
            out_specs=[SSPEC] * 2 + [VSPEC] * 8,
            out_shape=[
                pltpu.SMEM((1,), jnp.int32),
                plan.control_type,
                plan.held_type(inverse),
                plan.state_type,
                pltpu.VMEM((6 * LANES, LANES), jnp.bfloat16),
                pltpu.VMEM((SUB, LANES), jnp.int32),
            ] + [plan.pack_type] * 4,
            compiler_params=pltpu.CompilerParams(vmem_limit_bytes=VMEM_LIMIT),
            scratch_shapes=[
                pltpu.SMEM(color.shape, color.dtype),
                pltpu.SMEM(color.shape, color.dtype),
                pltpu.VMEM(rhs.shape, rhs.dtype),
                pltpu.VMEM(weights.shape, weights.dtype),
                pltpu.VMEM(neighbours.shape, neighbours.dtype),
                pltpu.VMEM(lists.shape, lists.dtype),
                plan.rest_type(inverse),
                pltpu.VMEM((pad, LANES), jnp.float32),
                pltpu.VMEM((pad, LANES), jnp.float32),
                pltpu.SemaphoreType.DMA((6,)),
                pltpu.SemaphoreType.DMA((CHUNKS,)),
            ],
        )(color, color_x, color_y, *(hbm(v) for v in (rhs, weights, neighbours, lists, inverse)))

    return call


def merge_kernel(plan, name, receives, steps):
    def kernel(*refs):
        old_state, *got = refs[:-1]
        state = refs[-1]
        del old_state
        odd_x = lax.axis_index("gx") & 1
        odd_y = lax.axis_index("gy") & 1

        @pl.when(receives(odd_x, odd_y))
        def _():
            for axis in sorted({axis for axis, _ in steps}):
                even, odd = (got[steps.index((axis, n))] for n in (0, 1))
                merge(plan, state, plan.along[axis], even, odd)

    def call(state, got):
        return pl.pallas_call(
            kernel,
            name=name,
            in_specs=[VSPEC] * (1 + len(got)),
            out_specs=VSPEC,
            out_shape=plan.state_type,
            input_output_aliases={0: 0},
            compiler_params=pltpu.CompilerParams(vmem_limit_bytes=VMEM_LIMIT),
        )(*(vmem(v) for v in (state, *got)))

    return call


def level_kernel(plan):
    def kernel(control, old_state, coupling, table, kept, inverse, state, xe, xo, ye, yo, rest, source, result, sems):
        del old_state
        steps = state[plan.step:plan.step + SUB, :] + 1.0
        state[plan.step:plan.step + SUB, :] = steps
        step = steps[0, 0].astype(jnp.int32)
        second = (step == control[SECOND]).astype(jnp.int32)
        turn = jnp.logical_or(step == control[FIRST], step == control[SECOND])

        @pl.when(turn)
        def _():
            update(plan, second, state, coupling, inverse, kept, rest, source, result, sems)

        for n, ref in enumerate((xe, xo, ye, yo)):
            write_pack(plan, state, table, n, ref)

    def call(control, state, coupling, table, kept, inverse):
        return pl.pallas_call(
            kernel,
            name="level",
            in_specs=[SSPEC] + [VSPEC] * 4 + [pl.BlockSpec(memory_space=pltpu.HBM)],
            out_specs=[VSPEC] * 5,
            out_shape=[plan.state_type] + [plan.pack_type] * 4,
            input_output_aliases={1: 0},
            compiler_params=pltpu.CompilerParams(vmem_limit_bytes=VMEM_LIMIT),
            scratch_shapes=[
                plan.rest_type(inverse),
                pltpu.VMEM((plan.pad, LANES), jnp.float32),
                pltpu.VMEM((plan.pad, LANES), jnp.float32),
                pltpu.SemaphoreType.DMA((CHUNKS,)),
            ],
        )(smem(control), *(vmem(v) for v in (state, coupling, table, kept)), hbm(inverse))

    return call


def last_kernel(plan):
    devices = plan.nx * plan.ny

    def kernel(state, out, sums):
        out[:, 0, :] = state[0:plan.rows, :]
        lane = lax.broadcasted_iota(jnp.int32, (devices, LANES), 1)
        first = jnp.sum(state[plan.norm:plan.norm + SUB, :])
        second = jnp.sum(state[plan.norm + SUB:plan.norm + 2 * SUB, :])
        sums[...] = jnp.where(lane == 0, first, jnp.where(lane == 1, second, 0.0))

    def call(state):
        return pl.pallas_call(
            kernel,
            name="last",
            in_specs=[VSPEC],
            out_specs=[VSPEC] * 2,
            out_shape=[
                pltpu.VMEM((plan.rows, 1, LANES), jnp.float32),
                pltpu.VMEM((devices, LANES), jnp.float32),
            ],
            compiler_params=pltpu.CompilerParams(vmem_limit_bytes=VMEM_LIMIT),
        )(vmem(state))

    return call


def edge_pairs(plan, axis, odd, sends, both):
    pairs = []
    for i in range(plan.nx):
        for j in range(plan.ny):
            step = 1 if (i, j)[axis] % 2 == odd else -1
            u, v = (i + step, j) if axis == 0 else (i, j + step)
            here = i * plan.ny + j
            if not (0 <= u < plan.nx and 0 <= v < plan.ny):
                if both:
                    pairs.append((here, here))
            elif both or sends(i, j):
                pairs.append((here, u * plan.ny + v))
    return pairs


def flow(plan, name, axes, parity):
    steps = [(axis, odd) for axis in (1, 0) if axis in axes for odd in (1, 0)]

    def sends(i, j):
        return (i * (0 in axes) + j * (1 in axes)) % 2 == parity

    def receives(i, j):
        return ((i if axes == (0,) else j if axes == (1,) else i ^ j) & 1) != parity

    def run(state, *packs):
        got = []
        for n, (axis, odd) in enumerate(steps):
            pairs = edge_pairs(plan, axis, odd, sends, n == len(steps) - 1)
            got.append(lax.ppermute(packs[2 * axis + odd], ("gx", "gy"), pairs))
        return merge_kernel(plan, name, receives, steps)(state, got)

    return run


def body_for(mesh):
    def body(rhs, inverse, weights, neighbours, send_lists, coloring):
        rows, faces = rhs.shape[1:]
        plan = Plan(mesh, rows, faces, send_lists.shape[2], weights.shape[1])
        color_x = lax.ppermute(coloring, "gx", [(i, i ^ 1) for i in range(plan.nx)])
        color_y = lax.ppermute(coloring, "gy", [(j, j ^ 1) for j in range(plan.ny)])
        code, control, kept, state, coupling, table, *packs = first_kernel(plan)(
            coloring, color_x, color_y, rhs.transpose(1, 0, 2), weights[0], neighbours[0], send_lists[0], inverse[0])
        flows = [
            flow(plan, "along_x0", (0,), 0),
            flow(plan, "along_y0", (1,), 0),
            flow(plan, "along_x1", (0,), 1),
            flow(plan, "along_y1", (1,), 1),
            flow(plan, "both0", (0, 1), 0),
            flow(plan, "both1", (0, 1), 1),
        ]

        def turn(carry):
            code, state, packs = carry
            state = lax.switch((code & 7) - 1, flows, state, *packs)
            state, *packs = level_kernel(plan)(control, state, coupling, table, kept, inverse[0])
            return code >> 4, state, tuple(packs)

        state = lax.while_loop(lambda carry: carry[0] != 0, turn, (code[0], state, tuple(packs)))[1]
        out, sums = last_kernel(plan)(state)
        sums = lax.all_to_all(sums, ("gx", "gy"), 0, 0, tiled=True)
        norms = jnp.sqrt(jnp.sum(sums[:, :2], axis=0))
        return out.transpose(1, 0, 2), norms

    return body


def solution(mesh):
    in_specs = (
        P("gx", None, "gy"),
        P("gx", None, None, "gy"),
        P("gx", None, "gy"),
        P("gx", None, "gy"),
        P("gx", None, "gy"),
        P("gx", "gy"),
    )
    out_specs = (P("gx", None, "gy"), P())
    return jax.shard_map(body_for(mesh), mesh=mesh, in_specs=in_specs, out_specs=out_specs, check_vma=False)
```

```python
import jax
import jax.numpy as jnp
from jax import lax
from jax.experimental import pallas as pl
from jax.experimental.pallas import tpu as pltpu
from jax.sharding import PartitionSpec as P

LANES = 128
SUB = 8
GROUP = 36
VMEM_LIMIT = 16 * 1024 * 1024
CHUNKS = 5
FIRST, SECOND, CONTROL = range(3)

VSPEC = pl.BlockSpec(memory_space=pltpu.VMEM)
SSPEC = pl.BlockSpec(memory_space=pltpu.SMEM)


def vmem(value):
    return pltpu.with_memory_space_constraint(value, pltpu.VMEM)


def hbm(value):
    return pltpu.with_memory_space_constraint(value, pltpu.HBM)


def smem(value):
    return pltpu.with_memory_space_constraint(value, pltpu.SMEM)


class Plan:
    def __init__(self, mesh, rows, faces, halo, neigh):
        self.nx, self.ny = mesh.shape["gx"], mesh.shape["gy"]
        self.rows, self.faces, self.halo, self.neigh = rows, faces, halo, neigh
        assert self.nx % 2 == 0 and self.ny % 2 == 0
        assert faces == LANES and 2 * halo == LANES
        self.tiles = -(-rows // (2 * SUB)) * 2
        self.pad = self.tiles * SUB
        self.half = self.pad // 2
        self.held = rows * 18 // 25 // CHUNKS * CHUNKS
        self.along = (self.pad, 2 * self.pad)
        self.rhs = 3 * self.pad
        self.norm = 4 * self.pad
        self.step = self.norm + 2 * SUB
        self.state = self.step + SUB
        self.state_type = pltpu.VMEM((self.state, LANES), jnp.float32)
        self.pack_type = pltpu.VMEM((self.half, LANES), jnp.float32)
        self.control_type = pltpu.SMEM((CONTROL,), jnp.int32)

    def held_type(self, inverse):
        return pltpu.VMEM((self.held, *inverse.shape[1:]), inverse.dtype)

    def rest_type(self, inverse):
        return pltpu.VMEM((self.rows - self.held, *inverse.shape[1:]), inverse.dtype)


def write_pack(plan, state, lists, row, ref):
    low = lax.broadcasted_iota(jnp.int32, (SUB, LANES), 1) < plan.halo
    index = jnp.broadcast_to(lists[pl.ds(row, 1), :], (SUB, LANES))

    def take(t):
        tile = state[t * SUB:(t + 1) * SUB, :]
        return jnp.take_along_axis(tile, index, axis=1, mode="promise_in_bounds")

    for t in range(plan.tiles // 2):
        ref[t * SUB:(t + 1) * SUB, :] = jnp.where(low, take(t), take(t + plan.tiles // 2))


def merge(plan, state, base, even, odd, there):
    low = lax.broadcasted_iota(jnp.int32, (SUB, LANES), 1) < plan.halo
    for t in range(plan.tiles // 2):
        a = even[t * SUB:(t + 1) * SUB, :]
        b = jnp.where(there, odd[t * SUB:(t + 1) * SUB, :], 0.0)
        first = jnp.where(low, a, pltpu.roll(b, plan.halo, 1))
        second = jnp.where(low, pltpu.roll(a, plan.halo, 1), b)
        state[pl.ds(base + t * SUB, SUB), :] = first
        state[pl.ds(base + plan.half + t * SUB, SUB), :] = second


def apply_inverse(plan, blocks, source, result, base, start, stop):
    src = source[0:plan.rows, :]
    group = max(g for g in range(1, GROUP + 1) if (stop - start) % g == 0)

    def step(n, carry):
        for k in range(group):
            i = start + n * group + k
            block = blocks[i].astype(jnp.float32)
            result[pl.ds(base + i, 1), :] = jnp.sum(block * src, axis=0, keepdims=True)
        return carry

    lax.fori_loop(0, (stop - start) // group, step, 0)


def pieces(plan):
    chunk = plan.held // CHUNKS
    return [(n * chunk, (n + 1) * chunk) for n in range(CHUNKS)] + [(plan.held, plan.rows)]


def piece_copy(plan, n, inverse, kept, rest, sem):
    start, stop = pieces(plan)[n]
    target = kept.at[pl.ds(start, stop - start)] if n < CHUNKS else rest
    return pltpu.make_async_copy(inverse.at[pl.ds(start, stop - start)], target, sem)


def parts_of(value):
    high = value.astype(jnp.bfloat16)
    low = (value - high.astype(jnp.float32)).astype(jnp.bfloat16)
    return high, low


def update(plan, second, state, coupling, inverse, kept, rest, source, result, sem):
    again = piece_copy(plan, CHUNKS, inverse, kept, rest, sem)
    again.start()
    pad = plan.pad
    values = jnp.concatenate([state[n * pad:(n + 1) * pad, :] for n in range(3)], axis=1)
    high, low = parts_of(values)
    size = 3 * LANES
    couple = jnp.dot(high, coupling[0:size, :], preferred_element_type=jnp.float32)
    couple = couple + jnp.dot(low, coupling[0:size, :], preferred_element_type=jnp.float32)
    couple = couple + jnp.dot(high, coupling[size:2 * size, :], preferred_element_type=jnp.float32)
    right = state[plan.rhs:plan.rhs + pad, :]
    source[...] = (right + couple).astype(jnp.bfloat16).astype(jnp.float32)
    result[pad - SUB:pad, :] = jnp.zeros((SUB, LANES), jnp.float32)
    apply_inverse(plan, kept, source, result, 0, 0, plan.held)
    again.wait()
    apply_inverse(plan, rest, source, result, plan.held, 0, plan.rows - plan.held)
    finish(plan, second, state, result)


def finish(plan, second, state, result):
    squares = jnp.zeros((SUB, LANES), jnp.float32)
    for t in range(plan.tiles):
        new = result[t * SUB:(t + 1) * SUB, :]
        delta = new - state[t * SUB:(t + 1) * SUB, :]
        squares = squares + delta * delta
        state[t * SUB:(t + 1) * SUB, :] = new
    state[pl.ds(pl.multiple_of(plan.norm + second * SUB, SUB), SUB), :] = squares


def prepare_kernel(plan):
    rows, pad, neigh = plan.rows, plan.pad, plan.neigh

    def kernel(rhs, weights, neighbours, lists, inverse, kept, state, coupling, table,
               rhs_v, weights_v, slots_v, lists_v, rest, source, result, sems, part_sems):
        moves = ((rhs, rhs_v), (neighbours, slots_v), (weights, weights_v), (lists, lists_v))
        copies = [pltpu.make_async_copy(a, b, sems.at[n]) for n, (a, b) in enumerate(moves)]
        parts = [piece_copy(plan, n, inverse, kept, rest, part_sems.at[n]) for n in range(CHUNKS + 1)]
        for c in copies + parts:
            c.start()
        odd_x = lax.axis_index("gx") & 1
        odd_y = lax.axis_index("gy") & 1
        state[...] = jnp.zeros(state.shape, jnp.float32)
        result[pad - SUB:pad, :] = jnp.zeros((SUB, LANES), jnp.float32)
        table[...] = jnp.zeros(table.shape, jnp.int32)
        for c in copies:
            c.wait()
        state[plan.rhs:plan.rhs + rows, :] = rhs_v[:, 0, :]
        source[...] = state[plan.rhs:plan.rhs + pad, :].astype(jnp.bfloat16).astype(jnp.float32)

        slots = slots_v[...]
        group = (slots - plan.faces) // plan.halo
        within = (slots - plan.faces) & (plan.halo - 1)
        along_y = (group >= 2).astype(jnp.int32)
        side = ((group & 1) + 1 + jnp.where(group >= 2, odd_y, odd_x)) & 1
        place = jnp.where(slots < plan.faces, slots, plan.faces * (1 + along_y) + within + plan.halo * side)
        size = 3 * LANES
        where = lax.broadcasted_iota(jnp.int32, (size, LANES), 0)
        total = jnp.zeros((size, LANES), jnp.float32)
        for k in range(neigh):
            total = total + jnp.where(where == place[k:k + 1, :], weights_v[k:k + 1, :], 0.0)
        coupling[0:size, :], coupling[size:2 * size, :] = parts_of(total)

        both = jnp.concatenate([lists_v[...], lists_v[...]], axis=1)
        for n, odd in ((0, odd_x), (2, odd_y)):
            table[n:n + 1, :] = jnp.where(odd == 0, both[n:n + 1], both[n + 1:n + 2])
            table[n + 1:n + 2, :] = jnp.where(odd == 0, both[n + 1:n + 2], both[n:n + 1])

        for n, (start, stop) in enumerate(pieces(plan)):
            parts[n].wait()
            if n < CHUNKS:
                apply_inverse(plan, kept, source, result, 0, start, stop)
            else:
                apply_inverse(plan, rest, source, result, start, 0, stop - start)
        finish(plan, 0, state, result)

    def call(rhs, weights, neighbours, lists, inverse):
        return pl.pallas_call(
            kernel,
            name="prepare",
            in_specs=[pl.BlockSpec(memory_space=pltpu.HBM)] * 5,
            out_specs=[VSPEC] * 4,
            out_shape=[
                plan.held_type(inverse),
                plan.state_type,
                pltpu.VMEM((6 * LANES, LANES), jnp.bfloat16),
                pltpu.VMEM((SUB, LANES), jnp.int32),
            ],
            compiler_params=pltpu.CompilerParams(vmem_limit_bytes=VMEM_LIMIT),
            scratch_shapes=[
                pltpu.VMEM(rhs.shape, rhs.dtype),
                pltpu.VMEM(weights.shape, weights.dtype),
                pltpu.VMEM(neighbours.shape, neighbours.dtype),
                pltpu.VMEM(lists.shape, lists.dtype),
                plan.rest_type(inverse),
                pltpu.VMEM((pad, LANES), jnp.float32),
                pltpu.VMEM((pad, LANES), jnp.float32),
                pltpu.SemaphoreType.DMA((4,)),
                pltpu.SemaphoreType.DMA((CHUNKS + 1,)),
            ],
        )(*(hbm(v) for v in (rhs, weights, neighbours, lists, inverse)))

    return call


def begin_kernel(plan):
    def kernel(color, color_x, color_y, old_state, table, code, control, state, xe, xo, ye, yo, cx, cy, sems):
        del old_state
        copies = [pltpu.make_async_copy(a, b, sems.at[n]) for n, (a, b) in enumerate(((color_x, cx), (color_y, cy)))]
        for c in copies:
            c.start()
        odd_x = lax.axis_index("gx") & 1
        odd_y = lax.axis_index("gy") & 1
        for c in copies:
            c.wait()
        mine, beside_x, beside_y = color[0, 0], cx[0, 0], cy[0, 0]
        across = 6 - mine - beside_x - beside_y
        to_x = jnp.logical_or(beside_x == 0, across == 0).astype(jnp.int32)
        to_y = jnp.logical_or(beside_y == 0, across == 0).astype(jnp.int32)
        zero_x, zero_y = odd_x ^ to_x, odd_y ^ to_y
        opposite = jnp.where(to_x == 0, jnp.where(to_y == 0, across, beside_x), jnp.where(to_y == 0, beside_y, mine))
        next_x = jnp.where(to_x == 0, jnp.where(to_y == 0, beside_x, across), jnp.where(to_y == 0, mine, beside_y))
        chain = opposite == 2
        first = jnp.where(chain, mine, jnp.where(opposite == 1, mine >> 1, (mine + 1) >> 1))
        control[FIRST] = first
        control[SECOND] = first + jnp.where(chain, 4, 2)
        red = zero_x ^ zero_y
        total = 0
        for n in range(7):
            step = n >> 1 & 1
            alternate = jnp.where(n < jnp.where(opposite == 1, 3, 4), 5 + (red ^ (n & 1)), 0)
            axis_x = 1 + 2 * (zero_x ^ step)
            axis_y = 2 + 2 * (zero_y ^ step)
            around = jnp.where((next_x == 1) == (n % 2 == 0), axis_x, axis_y)
            total = total + (jnp.where(chain, around, alternate) << (4 * n))
        code[0] = total

        @pl.when(first != 0)
        def _():
            state[0:plan.pad, :] = jnp.zeros((plan.pad, LANES), jnp.float32)
            state[plan.norm:plan.norm + SUB, :] = jnp.zeros((SUB, LANES), jnp.float32)

        for n, ref in enumerate((xe, xo, ye, yo)):
            write_pack(plan, state, table, n, ref)

    def call(color, color_x, color_y, state, table):
        return pl.pallas_call(
            kernel,
            name="begin",
            in_specs=[SSPEC] + [pl.BlockSpec(memory_space=pl.ANY)] * 2 + [VSPEC] * 2,
            out_specs=[SSPEC] * 2 + [VSPEC] * 5,
            out_shape=[pltpu.SMEM((1,), jnp.int32), plan.control_type, plan.state_type] + [plan.pack_type] * 4,
            input_output_aliases={3: 2},
            compiler_params=pltpu.CompilerParams(vmem_limit_bytes=VMEM_LIMIT),
            scratch_shapes=[
                pltpu.SMEM(color.shape, color.dtype),
                pltpu.SMEM(color.shape, color.dtype),
                pltpu.SemaphoreType.DMA((2,)),
            ],
        )(color, color_x, color_y, vmem(state), vmem(table))

    return call


def merge_kernel(plan, name, receives, steps):
    def kernel(*refs):
        old_state, *got = refs[:-1]
        state = refs[-1]
        del old_state
        place = (lax.axis_index("gx"), lax.axis_index("gy"))

        @pl.when(receives(place[0] & 1, place[1] & 1))
        def _():
            for axis in sorted({axis for axis, _ in steps}):
                even, odd = (got[steps.index((axis, n))] for n in (0, 1))
                there = jnp.logical_and(place[axis] > 0, place[axis] < (plan.nx, plan.ny)[axis] - 1)
                merge(plan, state, plan.along[axis], even, odd, there)

    def call(state, got):
        return pl.pallas_call(
            kernel,
            name=name,
            in_specs=[VSPEC] * (1 + len(got)),
            out_specs=VSPEC,
            out_shape=plan.state_type,
            input_output_aliases={0: 0},
            compiler_params=pltpu.CompilerParams(vmem_limit_bytes=VMEM_LIMIT),
        )(*(vmem(v) for v in (state, *got)))

    return call


def level_kernel(plan):
    def kernel(control, old_state, coupling, table, kept, inverse, state, xe, xo, ye, yo, rest, source, result, sem):
        del old_state
        steps = state[plan.step:plan.step + SUB, :] + 1.0
        state[plan.step:plan.step + SUB, :] = steps
        step = steps[0, 0].astype(jnp.int32)
        second = (step == control[SECOND]).astype(jnp.int32)
        turn = jnp.logical_or(step == control[FIRST], step == control[SECOND])

        @pl.when(turn)
        def _():
            update(plan, second, state, coupling, inverse, kept, rest, source, result, sem)

        for n, ref in enumerate((xe, xo, ye, yo)):
            write_pack(plan, state, table, n, ref)

    def call(control, state, coupling, table, kept, inverse):
        return pl.pallas_call(
            kernel,
            name="level",
            in_specs=[SSPEC] + [VSPEC] * 4 + [pl.BlockSpec(memory_space=pltpu.HBM)],
            out_specs=[VSPEC] * 5,
            out_shape=[plan.state_type] + [plan.pack_type] * 4,
            input_output_aliases={1: 0},
            compiler_params=pltpu.CompilerParams(vmem_limit_bytes=VMEM_LIMIT),
            scratch_shapes=[
                plan.rest_type(inverse),
                pltpu.VMEM((plan.pad, LANES), jnp.float32),
                pltpu.VMEM((plan.pad, LANES), jnp.float32),
                pltpu.SemaphoreType.DMA,
            ],
        )(smem(control), *(vmem(v) for v in (state, coupling, table, kept)), hbm(inverse))

    return call


def last_kernel(plan):
    devices = plan.nx * plan.ny

    def kernel(state, out, sums):
        out[:, 0, :] = state[0:plan.rows, :]
        lane = lax.broadcasted_iota(jnp.int32, (devices, LANES), 1)
        first = jnp.sum(state[plan.norm:plan.norm + SUB, :])
        second = jnp.sum(state[plan.norm + SUB:plan.norm + 2 * SUB, :])
        sums[...] = jnp.where(lane == 0, first, jnp.where(lane == 1, second, 0.0))

    def call(state):
        return pl.pallas_call(
            kernel,
            name="last",
            in_specs=[VSPEC],
            out_specs=[VSPEC] * 2,
            out_shape=[
                jax.ShapeDtypeStruct((plan.rows, 1, LANES), jnp.float32),
                pltpu.VMEM((devices, LANES), jnp.float32),
            ],
            compiler_params=pltpu.CompilerParams(vmem_limit_bytes=VMEM_LIMIT),
        )(vmem(state))

    return call


def edge_pairs(plan, axis, odd, sends, both):
    pairs = []
    for i in range(plan.nx):
        for j in range(plan.ny):
            step = 1 if (i, j)[axis] % 2 == odd else -1
            u, v = (i + step, j) if axis == 0 else (i, j + step)
            if 0 <= u < plan.nx and 0 <= v < plan.ny and (both or sends(i, j)):
                pairs.append((i * plan.ny + j, u * plan.ny + v))
    return pairs


def circle_pairs(plan, axis, parity):
    pairs = []

    def number(at):
        return at[0] * plan.ny + at[1]

    for i in range(plan.nx):
        for j in range(plan.ny):
            here = [i, j]
            ahead = 1 if here[axis] % 2 == 1 else -1
            inside = 0 <= here[axis] + ahead < (plan.nx, plan.ny)[axis]
            to = list(here)
            if inside:
                to[axis] += ahead
            if here[axis] % 2 != parity or not inside:
                to[1 - axis] ^= 1
            pairs.append((number(here), number(to)))
    return pairs


def flow(plan, name, axes, parity):
    steps = [(axis, odd) for axis in (1, 0) if axis in axes for odd in (1, 0)]

    def sends(i, j):
        return (i * (0 in axes) + j * (1 in axes)) % 2 == parity

    def receives(i, j):
        return ((i if axes == (0,) else j if axes == (1,) else i ^ j) & 1) != parity

    def run(state, *packs):
        got = []
        for n, (axis, odd) in enumerate(steps):
            if len(axes) == 1 and odd:
                pairs = circle_pairs(plan, axis, parity)
            else:
                pairs = edge_pairs(plan, axis, odd, sends, n == len(steps) - 1)
            got.append(lax.ppermute(packs[2 * axis + odd], ("gx", "gy"), pairs))
        return merge_kernel(plan, name, receives, steps)(state, got)

    return run


def body_for(mesh):
    def body(rhs, inverse, weights, neighbours, send_lists, coloring):
        rows, faces = rhs.shape[1:]
        plan = Plan(mesh, rows, faces, send_lists.shape[2], weights.shape[1])
        color_x = lax.ppermute(coloring, "gx", [(i, i ^ 1) for i in range(plan.nx)])
        color_y = lax.ppermute(coloring, "gy", [(j, j ^ 1) for j in range(plan.ny)])
        kept, state, coupling, table = prepare_kernel(plan)(
            rhs.transpose(1, 0, 2), weights[0], neighbours[0], send_lists[0], inverse[0])
        code, control, state, *packs = begin_kernel(plan)(coloring, color_x, color_y, state, table)
        flows = [
            flow(plan, f"along_{'xy'[axis]}{parity}", (axis,), parity)
            for parity in (0, 1) for axis in (0, 1)
        ]
        flows += [flow(plan, f"both{parity}", (0, 1), parity) for parity in (0, 1)]

        def turn(carry):
            code, state, packs = carry
            state = lax.switch((code & 7) - 1, flows, state, *packs)
            state, *packs = level_kernel(plan)(control, state, coupling, table, kept, inverse[0])
            return code >> 4, state, tuple(packs)

        state = lax.while_loop(lambda carry: carry[0] != 0, turn, (code[0], state, tuple(packs)))[1]
        out, sums = last_kernel(plan)(state)
        sums = lax.all_to_all(sums, ("gx", "gy"), 0, 0, tiled=True)
        norms = jnp.sqrt(jnp.sum(sums[:, :2], axis=0))
        return out.transpose(1, 0, 2), norms

    return body


def solution(mesh):
    in_specs = (
        P("gx", None, "gy"),
        P("gx", None, None, "gy"),
        P("gx", None, "gy"),
        P("gx", None, "gy"),
        P("gx", None, "gy"),
        P("gx", "gy"),
    )
    out_specs = (P("gx", None, "gy"), P())
    return jax.shard_map(body_for(mesh), mesh=mesh, in_specs=in_specs, out_specs=out_specs, check_vma=False)
```

```python
import jax
import jax.numpy as jnp
from jax import lax
from jax.experimental import pallas as pl
from jax.experimental.pallas import tpu as pltpu
from jax.sharding import PartitionSpec as P

LANES = 128
SUB = 8
GROUP = 36
VMEM_LIMIT = 16 * 1024 * 1024
CHUNKS = 5
FIRST, SECOND, CONTROL = range(3)

VSPEC = pl.BlockSpec(memory_space=pltpu.VMEM)
SSPEC = pl.BlockSpec(memory_space=pltpu.SMEM)


def vmem(value):
    return pltpu.with_memory_space_constraint(value, pltpu.VMEM)


def hbm(value):
    return pltpu.with_memory_space_constraint(value, pltpu.HBM)


def smem(value):
    return pltpu.with_memory_space_constraint(value, pltpu.SMEM)


class Plan:
    def __init__(self, mesh, rows, faces, halo, neigh):
        self.nx, self.ny = mesh.shape["gx"], mesh.shape["gy"]
        self.rows, self.faces, self.halo, self.neigh = rows, faces, halo, neigh
        assert self.nx % 2 == 0 and self.ny % 2 == 0
        assert faces == LANES and 2 * halo == LANES
        self.tiles = -(-rows // (2 * SUB)) * 2
        self.pad = self.tiles * SUB
        self.half = self.pad // 2
        self.held = rows * 18 // 25 // CHUNKS * CHUNKS
        self.along = (self.pad, 2 * self.pad)
        self.rhs = 3 * self.pad
        self.norm = 4 * self.pad
        self.step = self.norm + 2 * SUB
        self.state = self.step + SUB
        self.state_type = pltpu.VMEM((self.state, LANES), jnp.float32)
        self.pack_type = pltpu.VMEM((self.half, LANES), jnp.float32)
        self.control_type = pltpu.SMEM((CONTROL,), jnp.int32)

    def held_type(self, inverse):
        return pltpu.VMEM((self.held, *inverse.shape[1:]), inverse.dtype)

    def rest_type(self, inverse):
        return pltpu.VMEM((self.rows - self.held, *inverse.shape[1:]), inverse.dtype)


def write_pack(plan, state, lists, row, ref):
    low = lax.broadcasted_iota(jnp.int32, (SUB, LANES), 1) < plan.halo
    index = jnp.broadcast_to(lists[pl.ds(row, 1), :], (SUB, LANES))

    def take(t):
        tile = state[t * SUB:(t + 1) * SUB, :]
        return jnp.take_along_axis(tile, index, axis=1, mode="promise_in_bounds")

    for t in range(plan.tiles // 2):
        ref[t * SUB:(t + 1) * SUB, :] = jnp.where(low, take(t), take(t + plan.tiles // 2))


def merge(plan, state, base, even, odd, there):
    low = lax.broadcasted_iota(jnp.int32, (SUB, LANES), 1) < plan.halo
    for t in range(plan.tiles // 2):
        a = even[t * SUB:(t + 1) * SUB, :]
        b = jnp.where(there, odd[t * SUB:(t + 1) * SUB, :], 0.0)
        first = jnp.where(low, a, pltpu.roll(b, plan.halo, 1))
        second = jnp.where(low, pltpu.roll(a, plan.halo, 1), b)
        state[pl.ds(base + t * SUB, SUB), :] = first
        state[pl.ds(base + plan.half + t * SUB, SUB), :] = second


def apply_inverse(plan, blocks, source, result, base, start, stop):
    src = source[0:plan.rows, :]
    group = max(g for g in range(1, GROUP + 1) if (stop - start) % g == 0)

    def step(n, carry):
        for k in range(group):
            i = start + n * group + k
            block = blocks[i].astype(jnp.float32)
            result[pl.ds(base + i, 1), :] = jnp.sum(block * src, axis=0, keepdims=True)
        return carry

    lax.fori_loop(0, (stop - start) // group, step, 0)


def pieces(plan):
    chunk = plan.held // CHUNKS
    return [(n * chunk, (n + 1) * chunk) for n in range(CHUNKS)] + [(plan.held, plan.rows)]


def piece_copy(plan, n, inverse, kept, rest, sem):
    start, stop = pieces(plan)[n]
    target = kept.at[pl.ds(start, stop - start)] if n < CHUNKS else rest
    return pltpu.make_async_copy(inverse.at[pl.ds(start, stop - start)], target, sem)


def parts_of(value):
    high = value.astype(jnp.bfloat16)
    low = (value - high.astype(jnp.float32)).astype(jnp.bfloat16)
    return high, low


def update(plan, second, state, coupling, kept, rest, source, result):
    pad = plan.pad
    values = jnp.concatenate([state[n * pad:(n + 1) * pad, :] for n in range(3)], axis=1)
    high, low = parts_of(values)
    size = 3 * LANES
    couple = jnp.dot(high, coupling[0:size, :], preferred_element_type=jnp.float32)
    couple = couple + jnp.dot(low, coupling[0:size, :], preferred_element_type=jnp.float32)
    couple = couple + jnp.dot(high, coupling[size:2 * size, :], preferred_element_type=jnp.float32)
    right = state[plan.rhs:plan.rhs + pad, :]
    source[...] = (right + couple).astype(jnp.bfloat16).astype(jnp.float32)
    result[pad - SUB:pad, :] = jnp.zeros((SUB, LANES), jnp.float32)
    apply_inverse(plan, kept, source, result, 0, 0, plan.held)
    apply_inverse(plan, rest, source, result, plan.held, 0, plan.rows - plan.held)
    finish(plan, second, state, result)


def finish(plan, second, state, result):
    squares = jnp.zeros((SUB, LANES), jnp.float32)
    for t in range(plan.tiles):
        new = result[t * SUB:(t + 1) * SUB, :]
        delta = new - state[t * SUB:(t + 1) * SUB, :]
        squares = squares + delta * delta
        state[t * SUB:(t + 1) * SUB, :] = new
    state[pl.ds(pl.multiple_of(plan.norm + second * SUB, SUB), SUB), :] = squares


def prepare_kernel(plan):
    rows, pad, neigh = plan.rows, plan.pad, plan.neigh

    def kernel(rhs, weights, neighbours, lists, inverse, kept, state, coupling, table,
               rhs_v, weights_v, slots_v, lists_v, rest, source, result, sems, part_sems):
        moves = ((rhs, rhs_v), (neighbours, slots_v), (weights, weights_v), (lists, lists_v))
        copies = [pltpu.make_async_copy(a, b, sems.at[n]) for n, (a, b) in enumerate(moves)]
        parts = [piece_copy(plan, n, inverse, kept, rest, part_sems.at[n]) for n in range(CHUNKS + 1)]
        for c in copies + parts:
            c.start()
        odd_x = lax.axis_index("gx") & 1
        odd_y = lax.axis_index("gy") & 1
        state[...] = jnp.zeros(state.shape, jnp.float32)
        result[pad - SUB:pad, :] = jnp.zeros((SUB, LANES), jnp.float32)
        table[...] = jnp.zeros(table.shape, jnp.int32)
        for c in copies:
            c.wait()
        state[plan.rhs:plan.rhs + rows, :] = rhs_v[:, 0, :]
        source[...] = state[plan.rhs:plan.rhs + pad, :].astype(jnp.bfloat16).astype(jnp.float32)

        slots = slots_v[...]
        group = (slots - plan.faces) // plan.halo
        within = (slots - plan.faces) & (plan.halo - 1)
        along_y = (group >= 2).astype(jnp.int32)
        side = ((group & 1) + 1 + jnp.where(group >= 2, odd_y, odd_x)) & 1
        place = jnp.where(slots < plan.faces, slots, plan.faces * (1 + along_y) + within + plan.halo * side)
        size = 3 * LANES
        where = lax.broadcasted_iota(jnp.int32, (size, LANES), 0)
        total = jnp.zeros((size, LANES), jnp.float32)
        for k in range(neigh):
            total = total + jnp.where(where == place[k:k + 1, :], weights_v[k:k + 1, :], 0.0)
        coupling[0:size, :], coupling[size:2 * size, :] = parts_of(total)

        both = jnp.concatenate([lists_v[...], lists_v[...]], axis=1)
        for n, odd in ((0, odd_x), (2, odd_y)):
            table[n:n + 1, :] = jnp.where(odd == 0, both[n:n + 1], both[n + 1:n + 2])
            table[n + 1:n + 2, :] = jnp.where(odd == 0, both[n + 1:n + 2], both[n:n + 1])

        for n, (start, stop) in enumerate(pieces(plan)):
            parts[n].wait()
            if n < CHUNKS:
                apply_inverse(plan, kept, source, result, 0, start, stop)
            else:
                apply_inverse(plan, rest, source, result, start, 0, stop - start)
        finish(plan, 0, state, result)

    def call(rhs, weights, neighbours, lists, inverse):
        return pl.pallas_call(
            kernel,
            name="prepare",
            in_specs=[pl.BlockSpec(memory_space=pltpu.HBM)] * 5,
            out_specs=[VSPEC] * 4,
            out_shape=[
                plan.held_type(inverse),
                plan.state_type,
                pltpu.VMEM((6 * LANES, LANES), jnp.bfloat16),
                pltpu.VMEM((SUB, LANES), jnp.int32),
            ],
            compiler_params=pltpu.CompilerParams(vmem_limit_bytes=VMEM_LIMIT),
            scratch_shapes=[
                pltpu.VMEM(rhs.shape, rhs.dtype),
                pltpu.VMEM(weights.shape, weights.dtype),
                pltpu.VMEM(neighbours.shape, neighbours.dtype),
                pltpu.VMEM(lists.shape, lists.dtype),
                plan.rest_type(inverse),
                pltpu.VMEM((pad, LANES), jnp.float32),
                pltpu.VMEM((pad, LANES), jnp.float32),
                pltpu.SemaphoreType.DMA((4,)),
                pltpu.SemaphoreType.DMA((CHUNKS + 1,)),
            ],
        )(*(hbm(v) for v in (rhs, weights, neighbours, lists, inverse)))

    return call


def begin_kernel(plan):
    def kernel(color, color_x, color_y, old_state, table, code, control, state, xe, xo, ye, yo, cx, cy, sems):
        del old_state
        copies = [pltpu.make_async_copy(a, b, sems.at[n]) for n, (a, b) in enumerate(((color_x, cx), (color_y, cy)))]
        for c in copies:
            c.start()
        odd_x = lax.axis_index("gx") & 1
        odd_y = lax.axis_index("gy") & 1
        for c in copies:
            c.wait()
        mine, beside_x, beside_y = color[0, 0], cx[0, 0], cy[0, 0]
        across = 6 - mine - beside_x - beside_y
        to_x = jnp.logical_or(beside_x == 0, across == 0).astype(jnp.int32)
        to_y = jnp.logical_or(beside_y == 0, across == 0).astype(jnp.int32)
        zero_x, zero_y = odd_x ^ to_x, odd_y ^ to_y
        opposite = jnp.where(to_x == 0, jnp.where(to_y == 0, across, beside_x), jnp.where(to_y == 0, beside_y, mine))
        next_x = jnp.where(to_x == 0, jnp.where(to_y == 0, beside_x, across), jnp.where(to_y == 0, mine, beside_y))
        chain = opposite == 2
        first = jnp.where(chain, mine, jnp.where(opposite == 1, mine >> 1, (mine + 1) >> 1))
        control[FIRST] = first
        control[SECOND] = first + jnp.where(chain, 4, 2)
        red = zero_x ^ zero_y
        total = 0
        for n in range(7):
            step = n >> 1 & 1
            alternate = jnp.where(n < jnp.where(opposite == 1, 3, 4), 5 + (red ^ (n & 1)), 0)
            axis_x = 1 + 2 * (zero_x ^ step)
            axis_y = 2 + 2 * (zero_y ^ step)
            around = jnp.where((next_x == 1) == (n % 2 == 0), axis_x, axis_y)
            total = total + (jnp.where(chain, around, alternate) << (4 * n))
        code[0] = total

        @pl.when(first != 0)
        def _():
            state[0:plan.pad, :] = jnp.zeros((plan.pad, LANES), jnp.float32)
            state[plan.norm:plan.norm + SUB, :] = jnp.zeros((SUB, LANES), jnp.float32)

        for n, ref in enumerate((xe, xo, ye, yo)):
            write_pack(plan, state, table, n, ref)

    def call(color, color_x, color_y, state, table):
        return pl.pallas_call(
            kernel,
            name="begin",
            in_specs=[SSPEC] + [pl.BlockSpec(memory_space=pl.ANY)] * 2 + [VSPEC] * 2,
            out_specs=[SSPEC] * 2 + [VSPEC] * 5,
            out_shape=[pltpu.SMEM((1,), jnp.int32), plan.control_type, plan.state_type] + [plan.pack_type] * 4,
            input_output_aliases={3: 2},
            compiler_params=pltpu.CompilerParams(vmem_limit_bytes=VMEM_LIMIT),
            scratch_shapes=[
                pltpu.SMEM(color.shape, color.dtype),
                pltpu.SMEM(color.shape, color.dtype),
                pltpu.SemaphoreType.DMA((2,)),
            ],
        )(color, color_x, color_y, vmem(state), vmem(table))

    return call


def merge_kernel(plan, name, receives, steps):
    def kernel(*refs):
        old_state, *got = refs[:-1]
        state = refs[-1]
        del old_state
        place = (lax.axis_index("gx"), lax.axis_index("gy"))

        @pl.when(receives(place[0] & 1, place[1] & 1))
        def _():
            for axis in sorted({axis for axis, _ in steps}):
                even, odd = (got[steps.index((axis, n))] for n in (0, 1))
                there = jnp.logical_and(place[axis] > 0, place[axis] < (plan.nx, plan.ny)[axis] - 1)
                merge(plan, state, plan.along[axis], even, odd, there)

    def call(state, got):
        return pl.pallas_call(
            kernel,
            name=name,
            in_specs=[VSPEC] * (1 + len(got)),
            out_specs=VSPEC,
            out_shape=plan.state_type,
            input_output_aliases={0: 0},
            compiler_params=pltpu.CompilerParams(vmem_limit_bytes=VMEM_LIMIT),
        )(*(vmem(v) for v in (state, *got)))

    return call


def fetch_kernel(plan, name, receives):
    def kernel(inverse, rest, sem):
        @pl.when(receives(lax.axis_index("gx") & 1, lax.axis_index("gy") & 1))
        def _():
            copy = piece_copy(plan, CHUNKS, inverse, None, rest, sem)
            copy.start()
            copy.wait()

    def call(inverse):
        return pl.pallas_call(
            kernel,
            name=name,
            in_specs=[pl.BlockSpec(memory_space=pltpu.HBM)],
            out_specs=VSPEC,
            out_shape=plan.rest_type(inverse),
            compiler_params=pltpu.CompilerParams(vmem_limit_bytes=VMEM_LIMIT),
            scratch_shapes=[pltpu.SemaphoreType.DMA],
        )(hbm(inverse))

    return call


def level_kernel(plan):
    def kernel(control, old_state, coupling, table, kept, rest, state, xe, xo, ye, yo, source, result):
        del old_state
        steps = state[plan.step:plan.step + SUB, :] + 1.0
        state[plan.step:plan.step + SUB, :] = steps
        step = steps[0, 0].astype(jnp.int32)
        second = (step == control[SECOND]).astype(jnp.int32)
        turn = jnp.logical_or(step == control[FIRST], step == control[SECOND])

        @pl.when(turn)
        def _():
            update(plan, second, state, coupling, kept, rest, source, result)

        for n, ref in enumerate((xe, xo, ye, yo)):
            write_pack(plan, state, table, n, ref)

    def call(control, state, coupling, table, kept, rest):
        return pl.pallas_call(
            kernel,
            name="level",
            in_specs=[SSPEC] + [VSPEC] * 5,
            out_specs=[VSPEC] * 5,
            out_shape=[plan.state_type] + [plan.pack_type] * 4,
            input_output_aliases={1: 0},
            compiler_params=pltpu.CompilerParams(vmem_limit_bytes=VMEM_LIMIT),
            scratch_shapes=[
                pltpu.VMEM((plan.pad, LANES), jnp.float32),
                pltpu.VMEM((plan.pad, LANES), jnp.float32),
            ],
        )(smem(control), *(vmem(v) for v in (state, coupling, table, kept, rest)))

    return call


def last_kernel(plan):
    devices = plan.nx * plan.ny

    def kernel(state, out, sums):
        out[:, 0, :] = state[0:plan.rows, :]
        lane = lax.broadcasted_iota(jnp.int32, (devices, LANES), 1)
        first = jnp.sum(state[plan.norm:plan.norm + SUB, :])
        second = jnp.sum(state[plan.norm + SUB:plan.norm + 2 * SUB, :])
        sums[...] = jnp.where(lane == 0, first, jnp.where(lane == 1, second, 0.0))

    def call(state):
        return pl.pallas_call(
            kernel,
            name="last",
            in_specs=[VSPEC],
            out_specs=[VSPEC] * 2,
            out_shape=[
                jax.ShapeDtypeStruct((plan.rows, 1, LANES), jnp.float32),
                pltpu.VMEM((devices, LANES), jnp.float32),
            ],
            compiler_params=pltpu.CompilerParams(vmem_limit_bytes=VMEM_LIMIT),
        )(vmem(state))

    return call


def edge_pairs(plan, axis, odd, sends, both):
    pairs = []
    for i in range(plan.nx):
        for j in range(plan.ny):
            step = 1 if (i, j)[axis] % 2 == odd else -1
            u, v = (i + step, j) if axis == 0 else (i, j + step)
            if 0 <= u < plan.nx and 0 <= v < plan.ny and (both or sends(i, j)):
                pairs.append((i * plan.ny + j, u * plan.ny + v))
    return pairs


def circle_pairs(plan, axis, parity):
    pairs = []

    def number(at):
        return at[0] * plan.ny + at[1]

    for i in range(plan.nx):
        for j in range(plan.ny):
            here = [i, j]
            ahead = 1 if here[axis] % 2 == 1 else -1
            inside = 0 <= here[axis] + ahead < (plan.nx, plan.ny)[axis]
            to = list(here)
            if inside:
                to[axis] += ahead
            if here[axis] % 2 != parity or not inside:
                to[1 - axis] ^= 1
            pairs.append((number(here), number(to)))
    return pairs


def flow(plan, name, axes, parity):
    steps = [(axis, odd) for axis in (1, 0) if axis in axes for odd in (1, 0)]

    def sends(i, j):
        return (i * (0 in axes) + j * (1 in axes)) % 2 == parity

    def receives(i, j):
        return ((i if axes == (0,) else j if axes == (1,) else i ^ j) & 1) != parity

    def run(inverse, control, kept, coupling, table, state, *packs):
        got = []
        for n, (axis, odd) in enumerate(steps):
            if len(axes) == 1 and odd:
                pairs = circle_pairs(plan, axis, parity)
            else:
                pairs = edge_pairs(plan, axis, odd, sends, n == len(steps) - 1)
            got.append(lax.ppermute(packs[2 * axis + odd], ("gx", "gy"), pairs))
        rest = fetch_kernel(plan, f"fetch_{name}", receives)(inverse)
        state = merge_kernel(plan, name, receives, steps)(state, got)
        return tuple(level_kernel(plan)(control, state, coupling, table, kept, rest))

    return run


def body_for(mesh):
    def body(rhs, inverse, weights, neighbours, send_lists, coloring):
        rows, faces = rhs.shape[1:]
        plan = Plan(mesh, rows, faces, send_lists.shape[2], weights.shape[1])
        color_x = lax.ppermute(coloring, "gx", [(i, i ^ 1) for i in range(plan.nx)])
        color_y = lax.ppermute(coloring, "gy", [(j, j ^ 1) for j in range(plan.ny)])
        kept, state, coupling, table = prepare_kernel(plan)(
            rhs.transpose(1, 0, 2), weights[0], neighbours[0], send_lists[0], inverse[0])
        code, control, state, *packs = begin_kernel(plan)(coloring, color_x, color_y, state, table)
        flows = [
            flow(plan, f"along_{'xy'[axis]}{parity}", (axis,), parity)
            for parity in (0, 1) for axis in (0, 1)
        ]
        flows += [flow(plan, f"both{parity}", (0, 1), parity) for parity in (0, 1)]

        def turn(carry):
            code, state, packs = carry
            state, *packs = lax.switch(
                (code & 7) - 1, flows, inverse[0], control, kept, coupling, table, state, *packs)
            return code >> 4, state, tuple(packs)

        state = lax.while_loop(lambda carry: carry[0] != 0, turn, (code[0], state, tuple(packs)))[1]
        out, sums = last_kernel(plan)(state)
        sums = lax.all_to_all(sums, ("gx", "gy"), 0, 0, tiled=True)
        norms = jnp.sqrt(jnp.sum(sums[:, :2], axis=0))
        return out.transpose(1, 0, 2), norms

    return body


def solution(mesh):
    in_specs = (
        P("gx", None, "gy"),
        P("gx", None, None, "gy"),
        P("gx", None, "gy"),
        P("gx", None, "gy"),
        P("gx", None, "gy"),
        P("gx", "gy"),
    )
    out_specs = (P("gx", None, "gy"), P())
    return jax.shard_map(body_for(mesh), mesh=mesh, in_specs=in_specs, out_specs=out_specs, check_vma=False)
```

```python
import jax
import jax.numpy as jnp
from jax import lax
from jax.experimental import pallas as pl
from jax.experimental.pallas import tpu as pltpu
from jax.sharding import PartitionSpec as P

LANES = 128
SUB = 8
GROUP = 36
VMEM_LIMIT = 16 * 1024 * 1024
CHUNKS = 5
FIRST, SECOND, CONTROL = range(3)

VSPEC = pl.BlockSpec(memory_space=pltpu.VMEM)
SSPEC = pl.BlockSpec(memory_space=pltpu.SMEM)


def vmem(value):
    return pltpu.with_memory_space_constraint(value, pltpu.VMEM)


def hbm(value):
    return pltpu.with_memory_space_constraint(value, pltpu.HBM)


def smem(value):
    return pltpu.with_memory_space_constraint(value, pltpu.SMEM)


class Plan:
    def __init__(self, mesh, rows, faces, halo, neigh):
        self.nx, self.ny = mesh.shape["gx"], mesh.shape["gy"]
        self.rows, self.faces, self.halo, self.neigh = rows, faces, halo, neigh
        assert self.nx % 2 == 0 and self.ny % 2 == 0
        assert faces == LANES and 2 * halo == LANES
        self.tiles = -(-rows // (2 * SUB)) * 2
        self.pad = self.tiles * SUB
        self.half = self.pad // 2
        self.held = rows * 18 // 25 // CHUNKS * CHUNKS
        self.along = (self.pad, 2 * self.pad)
        self.rhs = 3 * self.pad
        self.norm = 4 * self.pad
        self.step = self.norm + 2 * SUB
        self.state = self.step + SUB
        self.state_type = pltpu.VMEM((self.state, LANES), jnp.float32)
        self.pack_type = pltpu.VMEM((self.half, LANES), jnp.float32)
        self.control_type = pltpu.SMEM((CONTROL,), jnp.int32)

    def held_type(self, inverse):
        return pltpu.VMEM((self.held, *inverse.shape[1:]), inverse.dtype)

    def rest_type(self, inverse):
        return pltpu.VMEM((self.rows - self.held, *inverse.shape[1:]), inverse.dtype)


def write_pack(plan, state, lists, row, ref):
    low = lax.broadcasted_iota(jnp.int32, (SUB, LANES), 1) < plan.halo
    index = jnp.broadcast_to(lists[pl.ds(row, 1), :], (SUB, LANES))

    def take(t):
        tile = state[t * SUB:(t + 1) * SUB, :]
        return jnp.take_along_axis(tile, index, axis=1, mode="promise_in_bounds")

    for t in range(plan.tiles // 2):
        ref[t * SUB:(t + 1) * SUB, :] = jnp.where(low, take(t), take(t + plan.tiles // 2))


def merge(plan, state, base, even, odd, there):
    low = lax.broadcasted_iota(jnp.int32, (SUB, LANES), 1) < plan.halo
    for t in range(plan.tiles // 2):
        a = even[t * SUB:(t + 1) * SUB, :]
        b = jnp.where(there, odd[t * SUB:(t + 1) * SUB, :], 0.0)
        first = jnp.where(low, a, pltpu.roll(b, plan.halo, 1))
        second = jnp.where(low, pltpu.roll(a, plan.halo, 1), b)
        state[pl.ds(base + t * SUB, SUB), :] = first
        state[pl.ds(base + plan.half + t * SUB, SUB), :] = second


def apply_inverse(plan, blocks, source, result, base, start, stop):
    src = source[0:plan.rows, :]
    group = max(g for g in range(1, GROUP + 1) if (stop - start) % g == 0)

    def step(n, carry):
        for k in range(group):
            i = start + n * group + k
            block = blocks[i].astype(jnp.float32)
            result[pl.ds(base + i, 1), :] = jnp.sum(block * src, axis=0, keepdims=True)
        return carry

    lax.fori_loop(0, (stop - start) // group, step, 0)


def pieces(plan):
    chunk = plan.held // CHUNKS
    return [(n * chunk, (n + 1) * chunk) for n in range(CHUNKS)] + [(plan.held, plan.rows)]


def piece_copy(plan, n, inverse, kept, rest, sem):
    start, stop = pieces(plan)[n]
    target = kept.at[pl.ds(start, stop - start)] if n < CHUNKS else rest
    return pltpu.make_async_copy(inverse.at[pl.ds(start, stop - start)], target, sem)


def parts_of(value):
    high = value.astype(jnp.bfloat16)
    low = (value - high.astype(jnp.float32)).astype(jnp.bfloat16)
    return high, low


def update(plan, second, state, coupling, kept, rest, source, result):
    pad = plan.pad
    values = jnp.concatenate([state[n * pad:(n + 1) * pad, :] for n in range(3)], axis=1)
    high, low = parts_of(values)
    size = 3 * LANES
    couple = jnp.dot(high, coupling[0:size, :], preferred_element_type=jnp.float32)
    couple = couple + jnp.dot(low, coupling[0:size, :], preferred_element_type=jnp.float32)
    couple = couple + jnp.dot(high, coupling[size:2 * size, :], preferred_element_type=jnp.float32)
    right = state[plan.rhs:plan.rhs + pad, :]
    source[...] = (right + couple).astype(jnp.bfloat16).astype(jnp.float32)
    result[pad - SUB:pad, :] = jnp.zeros((SUB, LANES), jnp.float32)
    apply_inverse(plan, kept, source, result, 0, 0, plan.held)
    apply_inverse(plan, rest, source, result, plan.held, 0, plan.rows - plan.held)
    finish(plan, second, state, result)


def finish(plan, second, state, result):
    squares = jnp.zeros((SUB, LANES), jnp.float32)
    for t in range(plan.tiles):
        new = result[t * SUB:(t + 1) * SUB, :]
        delta = new - state[t * SUB:(t + 1) * SUB, :]
        squares = squares + delta * delta
        state[t * SUB:(t + 1) * SUB, :] = new
    state[pl.ds(pl.multiple_of(plan.norm + second * SUB, SUB), SUB), :] = squares


def prepare_kernel(plan):
    rows, pad, neigh = plan.rows, plan.pad, plan.neigh

    def kernel(rhs, weights, neighbours, lists, inverse, kept, state, coupling, table,
               rhs_v, weights_v, slots_v, lists_v, rest, source, result, sems, part_sems):
        moves = ((rhs, rhs_v), (neighbours, slots_v), (weights, weights_v), (lists, lists_v))
        copies = [pltpu.make_async_copy(a, b, sems.at[n]) for n, (a, b) in enumerate(moves)]
        parts = [piece_copy(plan, n, inverse, kept, rest, part_sems.at[n]) for n in range(CHUNKS + 1)]
        for c in copies + parts:
            c.start()
        odd_x = lax.axis_index("gx") & 1
        odd_y = lax.axis_index("gy") & 1
        state[...] = jnp.zeros(state.shape, jnp.float32)
        result[pad - SUB:pad, :] = jnp.zeros((SUB, LANES), jnp.float32)
        table[...] = jnp.zeros(table.shape, jnp.int32)
        for c in copies:
            c.wait()
        state[plan.rhs:plan.rhs + rows, :] = rhs_v[:, 0, :]
        source[...] = state[plan.rhs:plan.rhs + pad, :].astype(jnp.bfloat16).astype(jnp.float32)

        slots = slots_v[...]
        group = (slots - plan.faces) // plan.halo
        within = (slots - plan.faces) & (plan.halo - 1)
        along_y = (group >= 2).astype(jnp.int32)
        side = ((group & 1) + 1 + jnp.where(group >= 2, odd_y, odd_x)) & 1
        place = jnp.where(slots < plan.faces, slots, plan.faces * (1 + along_y) + within + plan.halo * side)
        size = 3 * LANES
        where = lax.broadcasted_iota(jnp.int32, (size, LANES), 0)
        total = jnp.zeros((size, LANES), jnp.float32)
        for k in range(neigh):
            total = total + jnp.where(where == place[k:k + 1, :], weights_v[k:k + 1, :], 0.0)
        coupling[0:size, :], coupling[size:2 * size, :] = parts_of(total)

        both = jnp.concatenate([lists_v[...], lists_v[...]], axis=1)
        for n, odd in ((0, odd_x), (2, odd_y)):
            table[n:n + 1, :] = jnp.where(odd == 0, both[n:n + 1], both[n + 1:n + 2])
            table[n + 1:n + 2, :] = jnp.where(odd == 0, both[n + 1:n + 2], both[n:n + 1])

        for n, (start, stop) in enumerate(pieces(plan)):
            parts[n].wait()
            if n < CHUNKS:
                apply_inverse(plan, kept, source, result, 0, start, stop)
            else:
                apply_inverse(plan, rest, source, result, start, 0, stop - start)
        finish(plan, 0, state, result)

    def call(rhs, weights, neighbours, lists, inverse):
        return pl.pallas_call(
            kernel,
            name="prepare",
            in_specs=[pl.BlockSpec(memory_space=pltpu.HBM)] * 5,
            out_specs=[VSPEC] * 4,
            out_shape=[
                plan.held_type(inverse),
                plan.state_type,
                pltpu.VMEM((6 * LANES, LANES), jnp.bfloat16),
                pltpu.VMEM((SUB, LANES), jnp.int32),
            ],
            compiler_params=pltpu.CompilerParams(vmem_limit_bytes=VMEM_LIMIT),
            scratch_shapes=[
                pltpu.VMEM(rhs.shape, rhs.dtype),
                pltpu.VMEM(weights.shape, weights.dtype),
                pltpu.VMEM(neighbours.shape, neighbours.dtype),
                pltpu.VMEM(lists.shape, lists.dtype),
                plan.rest_type(inverse),
                pltpu.VMEM((pad, LANES), jnp.float32),
                pltpu.VMEM((pad, LANES), jnp.float32),
                pltpu.SemaphoreType.DMA((4,)),
                pltpu.SemaphoreType.DMA((CHUNKS + 1,)),
            ],
        )(*(hbm(v) for v in (rhs, weights, neighbours, lists, inverse)))

    return call


def begin_kernel(plan):
    def kernel(color, color_x, color_y, old_state, table, code, control, state, xe, xo, ye, yo, cx, cy, sems):
        del old_state
        copies = [pltpu.make_async_copy(a, b, sems.at[n]) for n, (a, b) in enumerate(((color_x, cx), (color_y, cy)))]
        for c in copies:
            c.start()
        odd_x = lax.axis_index("gx") & 1
        odd_y = lax.axis_index("gy") & 1
        for c in copies:
            c.wait()
        mine, beside_x, beside_y = color[0, 0], cx[0, 0], cy[0, 0]
        across = 6 - mine - beside_x - beside_y
        to_x = jnp.logical_or(beside_x == 0, across == 0).astype(jnp.int32)
        to_y = jnp.logical_or(beside_y == 0, across == 0).astype(jnp.int32)
        zero_x, zero_y = odd_x ^ to_x, odd_y ^ to_y
        opposite = jnp.where(to_x == 0, jnp.where(to_y == 0, across, beside_x), jnp.where(to_y == 0, beside_y, mine))
        next_x = jnp.where(to_x == 0, jnp.where(to_y == 0, beside_x, across), jnp.where(to_y == 0, mine, beside_y))
        chain = opposite == 2
        first = jnp.where(chain, mine, jnp.where(opposite == 1, mine >> 1, (mine + 1) >> 1))
        control[FIRST] = first
        control[SECOND] = first + jnp.where(chain, 4, 2)
        red = zero_x ^ zero_y
        total = 0
        for n in range(7):
            step = n >> 1 & 1
            alternate = jnp.where(n < jnp.where(opposite == 1, 3, 4), 5 + (red ^ (n & 1)), 0)
            axis_x = 1 + 2 * (zero_x ^ step)
            axis_y = 2 + 2 * (zero_y ^ step)
            around = jnp.where((next_x == 1) == (n % 2 == 0), axis_x, axis_y)
            total = total + (jnp.where(chain, around, alternate) << (4 * n))
        code[0] = total

        @pl.when(first != 0)
        def _():
            state[0:plan.pad, :] = jnp.zeros((plan.pad, LANES), jnp.float32)
            state[plan.norm:plan.norm + SUB, :] = jnp.zeros((SUB, LANES), jnp.float32)

        for n, ref in enumerate((xe, xo, ye, yo)):
            write_pack(plan, state, table, n, ref)

    def call(color, color_x, color_y, state, table):
        return pl.pallas_call(
            kernel,
            name="begin",
            in_specs=[SSPEC] + [pl.BlockSpec(memory_space=pl.ANY)] * 2 + [VSPEC] * 2,
            out_specs=[SSPEC] * 2 + [VSPEC] * 5,
            out_shape=[pltpu.SMEM((1,), jnp.int32), plan.control_type, plan.state_type] + [plan.pack_type] * 4,
            input_output_aliases={3: 2},
            compiler_params=pltpu.CompilerParams(vmem_limit_bytes=VMEM_LIMIT),
            scratch_shapes=[
                pltpu.SMEM(color.shape, color.dtype),
                pltpu.SMEM(color.shape, color.dtype),
                pltpu.SemaphoreType.DMA((2,)),
            ],
        )(color, color_x, color_y, vmem(state), vmem(table))

    return call


def fetch_kernel(plan, name, receives):
    def kernel(inverse, rest, sem):
        @pl.when(receives(lax.axis_index("gx") & 1, lax.axis_index("gy") & 1))
        def _():
            copy = piece_copy(plan, CHUNKS, inverse, None, rest, sem)
            copy.start()
            copy.wait()

    def call(inverse):
        return pl.pallas_call(
            kernel,
            name=name,
            in_specs=[pl.BlockSpec(memory_space=pltpu.HBM)],
            out_specs=VSPEC,
            out_shape=plan.rest_type(inverse),
            compiler_params=pltpu.CompilerParams(vmem_limit_bytes=VMEM_LIMIT),
            scratch_shapes=[pltpu.SemaphoreType.DMA],
        )(hbm(inverse))

    return call


def level_kernel(plan, name, receives, steps):
    def kernel(control, old_state, coupling, table, kept, rest, *refs):
        got = refs[:len(steps)]
        state, xe, xo, ye, yo, source, result = refs[len(steps):]
        del old_state
        at = (lax.axis_index("gx"), lax.axis_index("gy"))
        count = state[plan.step:plan.step + SUB, :] + 1.0
        state[plan.step:plan.step + SUB, :] = count

        @pl.when(receives(at[0] & 1, at[1] & 1))
        def _():
            for axis in sorted({axis for axis, _ in steps}):
                even, odd = (got[steps.index((axis, n))] for n in (0, 1))
                there = jnp.logical_and(at[axis] > 0, at[axis] < (plan.nx, plan.ny)[axis] - 1)
                merge(plan, state, plan.along[axis], even, odd, there)

            step = count[0, 0].astype(jnp.int32)
            second = (step == control[SECOND]).astype(jnp.int32)

            @pl.when(jnp.logical_or(step == control[FIRST], step == control[SECOND]))
            def _():
                update(plan, second, state, coupling, kept, rest, source, result)

        for n, ref in enumerate((xe, xo, ye, yo)):
            write_pack(plan, state, table, n, ref)

    def call(control, state, coupling, table, kept, rest, got):
        return pl.pallas_call(
            kernel,
            name=name,
            in_specs=[SSPEC] + [VSPEC] * (5 + len(got)),
            out_specs=[VSPEC] * 5,
            out_shape=[plan.state_type] + [plan.pack_type] * 4,
            input_output_aliases={1: 0},
            compiler_params=pltpu.CompilerParams(vmem_limit_bytes=VMEM_LIMIT),
            scratch_shapes=[
                pltpu.VMEM((plan.pad, LANES), jnp.float32),
                pltpu.VMEM((plan.pad, LANES), jnp.float32),
            ],
        )(smem(control), *(vmem(v) for v in (state, coupling, table, kept, rest, *got)))

    return call


def last_kernel(plan):
    devices = plan.nx * plan.ny

    def kernel(state, out, sums):
        out[:, 0, :] = state[0:plan.rows, :]
        lane = lax.broadcasted_iota(jnp.int32, (devices, LANES), 1)
        first = jnp.sum(state[plan.norm:plan.norm + SUB, :])
        second = jnp.sum(state[plan.norm + SUB:plan.norm + 2 * SUB, :])
        sums[...] = jnp.where(lane == 0, first, jnp.where(lane == 1, second, 0.0))

    def call(state):
        return pl.pallas_call(
            kernel,
            name="last",
            in_specs=[VSPEC],
            out_specs=[VSPEC] * 2,
            out_shape=[
                jax.ShapeDtypeStruct((plan.rows, 1, LANES), jnp.float32),
                pltpu.VMEM((devices, LANES), jnp.float32),
            ],
            compiler_params=pltpu.CompilerParams(vmem_limit_bytes=VMEM_LIMIT),
        )(vmem(state))

    return call


def edge_pairs(plan, axis, odd, sends, both):
    pairs = []
    for i in range(plan.nx):
        for j in range(plan.ny):
            step = 1 if (i, j)[axis] % 2 == odd else -1
            u, v = (i + step, j) if axis == 0 else (i, j + step)
            if 0 <= u < plan.nx and 0 <= v < plan.ny and (both or sends(i, j)):
                pairs.append((i * plan.ny + j, u * plan.ny + v))
    return pairs


def circle_pairs(plan, axis, parity):
    pairs = []

    def number(at):
        return at[0] * plan.ny + at[1]

    for i in range(plan.nx):
        for j in range(plan.ny):
            here = [i, j]
            ahead = 1 if here[axis] % 2 == 1 else -1
            inside = 0 <= here[axis] + ahead < (plan.nx, plan.ny)[axis]
            to = list(here)
            if inside:
                to[axis] += ahead
            if here[axis] % 2 != parity or not inside:
                to[1 - axis] ^= 1
            pairs.append((number(here), number(to)))
    return pairs


def flow(plan, name, axes, parity):
    steps = [(axis, odd) for axis in (1, 0) if axis in axes for odd in (1, 0)]

    def sends(i, j):
        return (i * (0 in axes) + j * (1 in axes)) % 2 == parity

    def receives(i, j):
        return ((i if axes == (0,) else j if axes == (1,) else i ^ j) & 1) != parity

    def run(inverse, control, kept, coupling, table, state, *packs):
        got = []
        for n, (axis, odd) in enumerate(steps):
            if len(axes) == 1 and odd:
                pairs = circle_pairs(plan, axis, parity)
            else:
                pairs = edge_pairs(plan, axis, odd, sends, n == len(steps) - 1)
            got.append(lax.ppermute(packs[2 * axis + odd], ("gx", "gy"), pairs))
        rest = fetch_kernel(plan, f"fetch_{name}", receives)(inverse)
        level = level_kernel(plan, name, receives, steps)
        return tuple(level(control, state, coupling, table, kept, rest, got))

    return run


def body_for(mesh):
    def body(rhs, inverse, weights, neighbours, send_lists, coloring):
        rows, faces = rhs.shape[1:]
        plan = Plan(mesh, rows, faces, send_lists.shape[2], weights.shape[1])
        color_x = lax.ppermute(coloring, "gx", [(i, i ^ 1) for i in range(plan.nx)])
        color_y = lax.ppermute(coloring, "gy", [(j, j ^ 1) for j in range(plan.ny)])
        kept, state, coupling, table = prepare_kernel(plan)(
            rhs.transpose(1, 0, 2), weights[0], neighbours[0], send_lists[0], inverse[0])
        code, control, state, *packs = begin_kernel(plan)(coloring, color_x, color_y, state, table)
        flows = [
            flow(plan, f"along_{'xy'[axis]}{parity}", (axis,), parity)
            for parity in (0, 1) for axis in (0, 1)
        ]
        flows += [flow(plan, f"both{parity}", (0, 1), parity) for parity in (0, 1)]

        def turn(carry):
            code, state, packs = carry
            state, *packs = lax.switch(
                (code & 7) - 1, flows, inverse[0], control, kept, coupling, table, state, *packs)
            return code >> 4, state, tuple(packs)

        state = lax.while_loop(lambda carry: carry[0] != 0, turn, (code[0], state, tuple(packs)))[1]
        out, sums = last_kernel(plan)(state)
        sums = lax.all_to_all(sums, ("gx", "gy"), 0, 0, tiled=True)
        norms = jnp.sqrt(jnp.sum(sums[:, :2], axis=0))
        return out.transpose(1, 0, 2), norms

    return body


def solution(mesh):
    in_specs = (
        P("gx", None, "gy"),
        P("gx", None, None, "gy"),
        P("gx", None, "gy"),
        P("gx", None, "gy"),
        P("gx", None, "gy"),
        P("gx", "gy"),
    )
    out_specs = (P("gx", None, "gy"), P())
    return jax.shard_map(body_for(mesh), mesh=mesh, in_specs=in_specs, out_specs=out_specs, check_vma=False)
```
